32 devices in a mesh: dp: 2 (over z, core), tp: 16 (over x, y).
Axes of the slice: x: 4, y: 4, z: 1, core: 2. Of those that a mesh axis runs over, the one named last changes fastest.
The devices are a block of a 4x4x8 slice.
Arguments:
- x: bfloat16 [5120, 7168], P(('dp', 'tp')), parts along dimension 0
- w_gate: bfloat16 [7168, 18432], P(None, 'tp')
- w_up: bfloat16 [7168, 18432], P(None, 'tp')
- w_down: bfloat16 [18432, 7168], P('tp')
Outputs:
- output: bfloat16 [5120, 7168], P(('dp', 'tp')), parts along dimension 0
There are 2 independent parts. The reference program is written for one: setup_inputs(seed, part) draws one part's arguments, and reference() takes and returns one part's arrays. A program takes and returns all parts, laid end to end along the dimension named above; an argument that names none is the same for every part.
All inputs are finite; a program needn't handle non-finite values.
Results may differ from the reference program's by a relative error of at most 0.016.
Values are sent between devices in bfloat16 or wider.
A program may use at most 768 MiB of HBM per device.

```python
import jax
import jax.numpy as jnp

ROWS = 2560
D = 7168
FF = 18432


def setup_inputs(seed: int = 0, part: int = 0) -> dict:
    kx, kg, ku, kd = jax.random.split(jax.random.key(seed), 4)
    drawn = {
        "x": jax.random.normal(jax.random.fold_in(kx, part), (ROWS, D), jnp.float32),
        "w_gate": jax.random.normal(kg, (D, FF), jnp.float32) * D**-0.5,
        "w_up": jax.random.normal(ku, (D, FF), jnp.float32) * D**-0.5,
        "w_down": jax.random.normal(kd, (FF, D), jnp.float32) * FF**-0.5,
    }
    return {k: v.astype(jnp.bfloat16) for k, v in drawn.items()}


def reference(x, w_gate, w_up, w_down):
    gate = jnp.dot(x, w_gate, preferred_element_type=jnp.float32)
    up = jnp.dot(x, w_up, preferred_element_type=jnp.float32)
    hidden = (jax.nn.silu(gate) * up).astype(jnp.bfloat16)
    return jnp.dot(hidden, w_down, preferred_element_type=jnp.float32).astype(jnp.bfloat16)
```

```python
import functools
import math

import jax
import jax.numpy as jnp
from jax import lax
from jax.experimental import pallas as pl
from jax.experimental.pallas import tpu as pltpu
from jax.sharding import PartitionSpec as P

MESH = pl.DeviceIdType.MESH
LANES = 128
EPOCHS = 2
OWN, OTHER = 0, 1
SLOTS = 8
TASK_SLOTS = ((0, 1, 2, 6), (3, 7, 4, 5))
GROUP_TILES = 3
LAG = 2
NB = 8
CHUNKS = 4
VLIM = 64600000


FIRST_U, BY_PARTNER = (14, 17), 2
TUNE = {'due_w': (95, 74), 'due_f': (70, 240), 'due_p': 815, 'due_h': (790, -30, 410, -30, 570, -170, 190, -130), 'backlog': 32.0, 'prefer': 438, 'phase': (1, 3, 3, 0.5)}


def columns(depth):
    t, (own, other) = depth // 28, FIRST_U
    end = 28 - BY_PARTNER
    return {
        OWN: ((0, own * t), (own * t, (28 - own) * t), None),
        OTHER: ((0, other * t), (other * t, (end - other) * t), (end * t, BY_PARTNER * t)),
    }


def gather_messages(depth, rows):
    msgs, deps = {}, {}
    re = rows // EPOCHS
    cols = columns(depth)

    def add(name, link, cls, src, dst, r, c, dep):
        msgs[name] = (link, cls, src, dst, r, c)
        deps[name] = dep

    for e in range(EPOCHS):
        every, a, b = (e * re, re), (e * re, re // 2), (e * re + re // 2, re // 2)
        add(("P1", OTHER, e), "P", OWN, 0, 0, every, cols[OTHER][0], [])
        add(("P2", OTHER, e), "P", OWN, 0, 0, every, (cols[OTHER][1][0], depth - cols[OTHER][1][0]), [])
        for cls in (OWN, OTHER):
            u, y, _ = cols[cls]
            m = lambda name: (name, cls, e)
            own_u = [] if cls == OWN else [("P1", OTHER, e)]
            own_y = [] if cls == OWN else [("P2", OTHER, e)]
            add(m("U1"), "U", cls, 0, 1, every, u, own_u)
            add(m("N1"), "N", cls, 0, 6, every, u, own_u)
            add(m("S1"), "S", cls, 0, 2, every, u, own_u)
            add(m("U2"), "U", cls, 0, 1, every, y, own_y)
            add(m("N2"), "N", cls, 0, 6, every, y, own_y)
            add(m("S2"), "S", cls, 0, 2, every, y, own_y)
            add(m("N3"), "N", cls, 1, 7, every, u, [m("U1")])
            add(m("S3"), "S", cls, 1, 3, every, u, [m("U1")])
            add(m("N4"), "N", cls, 6, 4, a, u, [m("N1")])
            add(m("S4"), "S", cls, 2, 4, b, u, [m("S1")])
            add(m("N5"), "N", cls, 6, 4, a, y, [m("N2")])
            add(m("S5"), "S", cls, 2, 4, b, y, [m("S2")])
            add(m("U3"), "U", cls, 6, 7, every, y, [m("N2")])
            add(m("U4"), "U", cls, 2, 3, every, y, [m("S2")])
            add(m("N6"), "N", cls, 7, 5, a, u, [m("N3")])
            add(m("S6"), "S", cls, 3, 5, b, u, [m("S3")])
            add(m("U5"), "U", cls, 4, 5, a, y, [m("N5")])
            add(m("U6"), "U", cls, 4, 5, b, y, [m("S5")])
        last = {1: ["U2"], 6: ["N2"], 2: ["S2"], 7: ["U3"], 3: ["U4"], 4: ["N5", "S5"], 5: ["U5", "U6"]}
        for s, need in last.items():
            add((f"F{s}", OTHER, e), "P", OWN, s, s, every, cols[OTHER][2], [(n, OWN, e) for n in need])
    return msgs, deps


def kind_of(message):
    to, cls, _, _, (_, r), cols = message
    return "P" if to == "P" else cls, r, cols


def send_kinds(msgs):
    return sorted({kind_of(m) for m in msgs.values()}, key=str)


def plan(depth, rows, width):
    rate, delay, tile_us, gt = 46.6e3, 2.2, 1.46, GROUP_TILES
    due_w, due_f, due_p, due_h, backlog = (TUNE[k] for k in ("due_w", "due_f", "due_p", "due_h", "backlog"))
    msgs, deps = gather_messages(depth, rows)
    pending = {name: set(d) for name, d in deps.items()}
    lack = {}
    for name, (link, cls, src, dst, r, c) in msgs.items():
        where = (OTHER if link == "P" else cls, name[2], dst)
        lack.setdefault(where, set()).add(name)
    pieces = depth // 4 // 256
    tasks = [(cls, e, h) for e in range(EPOCHS) for cls in (OWN, OTHER) for h in range(2)]
    subs = width // LANES // gt
    re, unit = rows // EPOCHS, depth // 28
    ncu, ncy = 8 * unit // CHUNKS, 6 * unit // CHUNKS
    nsteps = 2 * EPOCHS * CHUNKS
    copies = {}
    for i, (name, (link, cls, _, dst, (_, r), (_, c))) in enumerate(msgs.items()):
        e = name[2]
        if name[0][0] == "P":
            rank = due_p * e
        elif name[0][0] == "F":
            rank = due_f[e] + (15 if dst in TASK_SLOTS[1] else 0)
        else:
            rank = TUNE["phase"][2 * e + cls] * 1000 + i
        copies[name] = (link, r * c * 2, rank)
    for k in range(pieces):
        copies["W", k] = ("P", width * 256 * 2, due_w[0] + due_w[1] * k)
    for t in range(len(tasks)):
        copies["H", t] = ("P", 4 * re * width * 2, due_h[t] + 10 * t)
    parts = {
        0: ("N", re * ncu), 1: ("S", re * ncu), 2: ("U", 4 * re * ncy),
        3: ("N", 2 * re * ncu), 4: ("S", 2 * re * ncu), 5: ("N", re // 2 * ncy), 6: ("S", re // 2 * ncy),
        7: ("U", re * ncu), 8: ("N", re * ncy), 9: ("S", re * ncy),
    }
    stages = (((0, 1, 2), 1.65, ()), ((3, 4, 5, 6), 1.75, (0, 1, 2)), ((7, 8, 9), 1.35, (3, 4, 5, 6)), ((), 1.0, (7, 8, 9)))
    free = dict.fromkeys("NSUPC", 0.0)
    avail = [n for n in msgs if not pending[n]] + [("W", k) for k in range(pieces)]
    now, arrivals = 0.0, []
    arrived = {}
    steps, ops = [], []
    loaded = {}
    task = sub = it = forwarded = 0

    def emit(*op):
        ops.append(op)

    def post(link, nbytes, what, at=None):
        free[link] = max(now if at is None else at, free[link]) + nbytes / (rate if link != "C" else 300e3)
        arrived[what] = free[link] + delay
        if what[0] not in "DHBE":
            arrivals.append((free[link] + delay, what))

    def issue():
        for n in sorted(avail, key=lambda n: copies[n][2]):
            link, nbytes, _ = copies[n]
            if free[link] - now < backlog:
                avail.remove(n)
                emit({"W": "wsend", "H": "hsend"}.get(n[0], "send"), n[1] if n[0] in "WH" else n)
                post(link, nbytes, n)
        for k in range(task, min(task + 2, len(tasks))):
            cls, e, h = tasks[k]
            for i, s in enumerate(TASK_SLOTS[h]):
                if (k, i) not in loaded and not lack.get((cls, e, s)):
                    loaded[k, i] = now + 1.5
                    emit("load", k, i)

    INF = 1e9

    def b_ready():
        t = 0.0
        if it < nsteps:
            g = it // CHUNKS
            if it % CHUNKS == 0:
                e, cls = g // 2, 1 - g % 2
                if task <= e * 4 + cls * 2 + 1 or forwarded < pieces:
                    return INF
                for k in range(2):
                    t = max(t, arrived.get(("H", 2 * g + k), INF))
            if it == 0:
                t = max(t, max(arrived["D", k] for k in range(pieces)))
        for j in (1, 2, 3):
            s = it - j * LAG
            if 0 <= s < nsteps:
                for k in stages[j][2]:
                    t = max(t, arrived["B", k, s])
        return t

    while task < len(tasks) or it < nsteps + 3 * LAG:
        issue()
        for a in sorted((a for a in arrivals if a[0] <= now), key=lambda a: a[0]):
            arrivals.remove(a)
            what = a[1]
            now += 0.03
            emit("recv", what)
            if what[0] == "W":
                emit("forward", what[1])
                forwarded += 1
                post("C", width * 256 * 2, ("D", what[1]))
            else:
                for s in lack.values():
                    s.discard(what)
                for n in msgs:
                    if what in pending[n]:
                        pending[n].discard(what)
                        if not pending[n]:
                            avail.append(n)
            issue()
        tile_at = INF
        if task < len(tasks) and all((task, i) in loaded for i in range(4)):
            tile_at = max(loaded[task, i] for i in range(4))
        b_at = b_ready() if it < nsteps + 3 * LAG else INF
        choice = None
        if b_at <= now and tile_at <= now:
            busy = min(free["N"], free["U"]) - now
            choice = "B" if busy < TUNE["prefer"] else "T"
        elif b_at <= now:
            choice = "B"
        elif tile_at <= now:
            choice = "T"
        if choice == "T":
            steps.append((ops, "T"))
            ops = []
            now += gt * tile_us
            sub += 1
            if sub == subs:
                avail.append(("H", task))
                task, sub = task + 1, 0
            continue
        if choice == "B":
            steps.append((ops, "B"))
            ops = []
            for j in (3, 2, 1, 0):
                s = it - j * LAG
                if 0 <= s < nsteps:
                    now += stages[j][1]
                    for k in stages[j][0]:
                        link, n = parts[k]
                        post(link, 2 * n, ("B", k, s))
                    if j == 3 and s // CHUNKS % 2 == 0:
                        post("P", 2 * re * (ncu + ncy), ("E", s))
            now += 0.1
            it += 1
            continue
        times = [a[0] for a in arrivals] + [t for t in (tile_at, b_at) if t < INF]
        if avail:
            times.append(min(max(now + 0.3, free[copies[n][0]] - backlog + 0.1) for n in avail))
        now = max(now, min(times))
    assert not avail and not arrivals, (avail, arrivals)
    steps.append((ops, ""))
    return steps


def kernel(n, steps_, msgs, x_hbm, gate_hbm, up_hbm, down_hbm, out, xl, gbuf, w, xbuf, hid,
           lu1, lu2, lu3, ly1, ly2, ly3, tu1, tu2, tu3, ty1, ty2, ty3, tq,
           gsend, grecv, xsem, gusem, wosem, wsend, wrecv, dsend, drecv, hsend, hrecv,
           bsend, brecv, fsend, frecv):
    rows, depth = x_hbm.shape
    width = gate_hbm.shape[1]
    re, half = rows // EPOCHS, depth // 2
    quarter, hr = half // 2, re // 2
    tiles = width // LANES
    pieces = quarter // 256
    unit = depth // 28
    ncu, ncy = 8 * unit // CHUNKS, 6 * unit // CHUNKS
    tasks = [(cls, e, h) for e in range(EPOCHS) for cls in (OWN, OTHER) for h in range(2)]
    total_tiles = len(tasks) * tiles
    steps = 2 * EPOCHS * CHUNKS

    side = math.isqrt(n)
    me, dp = lax.axis_index("tp"), lax.axis_index("dp")
    x, y = me // side, me % side
    role, core = ((x + 1) // 2) % 2, dp % 2
    link = {
        "N": {"tp": x * side + (y + 1) % side},
        "S": {"tp": x * side + (y + side - 1) % side},
        "U": {"tp": (side - 1 - x) * side + y},
        "P": {"tp": (x + 1 - 2 * (x % 2)) * side + y},
        "C": {"dp": dp + 1 - 2 * core},
    }

    def remote(src, dst, ssem, rsem, to):
        return pltpu.make_async_remote_copy(
            src_ref=src, dst_ref=dst, send_sem=ssem, recv_sem=rsem, device_id=link[to], device_id_type=MESH
        )

    def sent(ref, sem):
        pltpu.make_async_copy(ref, ref, sem).wait()

    def signal(sem, to):
        pl.semaphore_signal(sem, inc=1, device_id=link[to], device_id_type=MESH)

    barrier = pltpu.get_barrier_semaphore()
    for to in link:
        signal(barrier, to)

    index = {name: i for i, name in enumerate(msgs)}
    kinds = send_kinds(msgs)

    def kind(name):
        return kind_of(msgs[name])

    def source(cls, slot):
        return x_hbm if cls == OWN and slot == 0 else xl.at[cls, slot]

    def gcopy(name):
        to, cls, src, dst, (r, nr), (c, nc) = msgs[name]
        there = OTHER if to == "P" else cls
        block = (pl.ds(r, nr), pl.ds(c, nc))
        return remote(
            source(cls, src).at[block], xl.at[(there, dst, *block)], gsend.at[kinds.index(kind(name))], grecv.at[index[name]], to
        )

    def xload(t, i):
        cls, e, h = tasks[t]
        src = source(cls, TASK_SLOTS[h][i]).at[pl.ds(e * re, re)]
        return pltpu.make_async_copy(src, xbuf.at[t % 2, pl.ds(i * re, re)], xsem.at[t % 2])

    def load_tile(k):
        slot = lax.rem(k, 3)
        cols = pl.ds(pl.multiple_of(lax.rem(k, tiles) * LANES, LANES), LANES)
        return (
            pltpu.make_async_copy(gate_hbm.at[:, cols], gbuf.at[slot, :, pl.ds(0, LANES)], gusem.at[slot]),
            pltpu.make_async_copy(up_hbm.at[:, cols], gbuf.at[slot, :, pl.ds(LANES, LANES)], gusem.at[slot]),
        )

    def wcopy(k):
        there = pl.ds(pl.multiple_of(core * quarter + k * 256, LANES), 256)
        here = pl.ds(pl.multiple_of((1 - role) * half + core * quarter + k * 256, LANES), 256)
        return remote(down_hbm.at[:, here], w.at[pl.ds(width, width), there], wsend, wrecv.at[k], "P")

    def dcopy(k, whose):
        cols = pl.ds(pl.multiple_of(whose * quarter + k * 256, LANES), 256)
        block = w.at[pl.ds(width, width), cols]
        return remote(block, block, dsend, drecv, "C")

    def hcopy(t, i):
        cls, e, h = tasks[t]
        slot = TASK_SLOTS[h][i]
        src = hid.at[(2 * e + 1 - cls) * SLOTS + slot, :, pl.ds(0, width)]
        dst = hid.at[(2 * e + cls) * SLOTS + slot, :, pl.ds(width, width)]
        return remote(src, dst, hsend, hrecv.at[t], "P")

    def do(op):
        kind, what = op[0], op[1]
        if kind == "send":
            gcopy(what).start()
        elif kind == "recv" and what[0] == "W":
            wcopy(what[1]).wait_recv()
        elif kind == "recv":
            gcopy(what).wait_recv()
        elif kind == "load":
            xload(what, op[2]).start()
        elif kind == "wsend":
            wcopy(what).start()
        elif kind == "forward":
            dcopy(what, core).start()
        elif kind == "hsend":
            for i in range(4):
                hcopy(what, i).start()

    def communicate(j):
        for k, (ops, _) in enumerate(steps_):
            if ops:

                @pl.when(j == k)
                def _():
                    for op in ops:
                        do(op)

    def tile(k):
        t, i, slot = k // tiles, lax.rem(k, tiles), lax.rem(k, 3)
        cls, e, h = lax.rem(t // 2, 2), t // 4, lax.rem(t, 2)
        b = lax.rem(t, 2)

        @pl.when(i == 0)
        def _():
            sent(xbuf.at[b], xsem.at[b])

        sent(gbuf.at[slot], gusem.at[slot])

        @pl.when(k + 2 < total_tiles)
        def _():
            for c in load_tile(k + 2):
                c.start()

        acc = jnp.dot(xbuf[b], gbuf[slot], preferred_element_type=jnp.float32)
        gate, up = acc[:, :LANES], acc[:, LANES:]
        h_tile = (jax.nn.silu(gate) * up).astype(hid.dtype)
        cols = pl.ds(pl.multiple_of(i * LANES, LANES), LANES)
        for j in range(4):
            place = TASK_SLOTS[0][j] + h * (TASK_SLOTS[1][j] - TASK_SLOTS[0][j])
            hid[(2 * e + 1 - cls) * SLOTS + place, :, cols] = h_tile[j * re : (j + 1) * re]

    def work(g):
        def one(i, _):
            tile(g * GROUP_TILES + i)
            return 0

        lax.fori_loop(0, GROUP_TILES, one, 0)

    pl.semaphore_wait(barrier, len(link))
    for c in load_tile(0) + load_tile(1):
        c.start()
    load_w = pltpu.make_async_copy(
        down_hbm.at[:, pl.ds(pl.multiple_of(role * half, LANES), half)], w.at[pl.ds(0, width)], wosem
    )
    load_w.start()

    def term(g, slots, start, size):
        out_rows = len(slots) * re
        if slots == tuple(range(slots[0], slots[0] + len(slots))):
            lhs = hid[pl.ds(g * SLOTS + slots[0], len(slots))].reshape(out_rows, 2 * width)
        else:
            lhs = jnp.concatenate([hid[g * SLOTS + s] for s in slots], axis=0)
        return jnp.dot(lhs, w[:, pl.ds(pl.multiple_of(start, LANES), size)], preferred_element_type=jnp.float32)

    f32 = lambda v: v.astype(jnp.float32)
    bf = lambda v: v.astype(jnp.bfloat16)

    def place(s):
        c = lax.rem(s, CHUNKS)
        return s // CHUNKS, c * ncu, 8 * unit + c * ncy, lax.rem(s, NB), lax.rem(s, 2)

    table = (
        ("N", tu1, 0, 0, lu1), ("S", tu1, 0, 1, lu1), ("U", ty1, 1, None, ly1),
        ("N", tu2, 2, 0, lu2), ("S", tu2, 2, 1, lu2), ("N", ty2, 3, 0, ly2), ("S", ty2, 3, 1, ly2),
        ("U", tu3, 4, None, lu3), ("N", ty3, 5, 0, ly3), ("S", ty3, 5, 1, ly3),
    )

    def bcopy(k, s):
        _, _, _, sl, st = place(s)
        to, staging, i, part, landing = table[k]
        src, dst = (staging.at[st], landing.at[sl]) if part is None else (staging.at[st, part], landing.at[sl, part])
        return remote(src, dst, bsend.at[st, i], brecv.at[lax.rem(s, 4), k], to)

    def left(s, k):
        _, staging, i, _, _ = table[k]
        st = lax.rem(s, 2)
        sent(staging.at[st], bsend.at[st, i])

    def free_staging(s, copies):
        @pl.when(s >= 2)
        def _():
            for k in copies:
                left(s - 2, k)

    def arrived(s, kinds):
        for k in kinds:
            bcopy(k, s).wait_recv()

    def stage1(s):
        g, cu, cy, sl, st = place(s)

        @pl.when(lax.rem(s, CHUNKS) == 0)
        def _():
            for h in range(2):
                sent(hid.at[pl.ds(g * SLOTS, 4), :, pl.ds(width, width)], hrecv.at[2 * g + h])

        free_staging(s, (0, 2))
        t = term(g, (4, 5), cu, ncu).reshape(2, re, ncu)
        tu1[st, 0] = bf(t[:, :hr])
        tu1[st, 1] = bf(t[:, hr:])
        for k in (0, 1):
            bcopy(k, s).start()
        t = term(g, (1, 3, 5, 7), cy, ncy)
        ty1[st] = bf(t).reshape(4, re, ncy)
        bcopy(2, s).start()

    def stage2(s):
        g, cu, cy, sl, st = place(s)
        arrived(s, (0, 1, 2))
        free_staging(s, (3, 5))
        t = term(g, (2, 3), cu, ncu).reshape(2, re, ncu)
        tu2[st, 0, :, :hr] = bf(t[:, :hr] + f32(lu1[sl, 0]))
        tu2[st, 0, :, hr:] = bf(t[:, hr:])
        bcopy(3, s).start()
        t = term(g, (6, 7), cu, ncu).reshape(2, re, ncu)
        tu2[st, 1, :, :hr] = bf(t[:, :hr])
        tu2[st, 1, :, hr:] = bf(t[:, hr:] + f32(lu1[sl, 1]))
        bcopy(4, s).start()
        t = term(g, (4,), cy, ncy) + f32(ly1[sl, 2])
        ty2[st, 0] = bf(t[:hr])
        ty2[st, 1] = bf(t[hr:])
        for k in (5, 6):
            bcopy(k, s).start()

    def stage3(s):
        g, cu, cy, sl, st = place(s)
        arrived(s, (3, 4, 5, 6))
        free_staging(s, (7, 8))
        t = term(g, (1,), cu, ncu)
        tu3[st] = bf(t + f32(lu2[sl, 0, 1]) + f32(lu2[sl, 1, 1]))
        bcopy(7, s).start()
        t = term(g, (2,), cy, ncy) + f32(ly1[sl, 1])
        ty3[st, 0, :hr] = bf(t[:hr] + f32(ly2[sl, 0]))
        ty3[st, 0, hr:] = bf(t[hr:])
        t = term(g, (6,), cy, ncy) + f32(ly1[sl, 3])
        ty3[st, 1, :hr] = bf(t[:hr])
        ty3[st, 1, hr:] = bf(t[hr:] + f32(ly2[sl, 1]))
        for k in (8, 9):
            bcopy(k, s).start()

    def fcopy(s, k):
        g, cu, cy, _, st = place(s)
        start, size = ((cu, ncu), (cy, ncy))[k]
        r = pl.ds(pl.multiple_of((g // 2) * re, 8), re)
        cols = pl.ds(pl.multiple_of(role * half + start, LANES), size)
        c = lax.rem(s, CHUNKS)
        return remote(tq.at[c, :, pl.ds(k * ncu, size)], out.at[r, cols], fsend.at[c], frecv.at[g // 2], "P")

    def stage4(s):
        g, cu, cy, sl, st = place(s)
        e, c = g // 2, lax.rem(s, CHUNKS)
        arrived(s, (7, 8, 9))

        @pl.when(lax.rem(g, 2) == 0)
        def _():
            @pl.when(e > 0)
            def _():
                sent(tq.at[c], fsend.at[c])

        tu = term(g, (0,), cu, ncu) + f32(lu2[sl, 0, 0]) + f32(lu2[sl, 1, 0]) + f32(lu3[sl])
        ty = term(g, (0,), cy, ncy) + f32(ly1[sl, 0]) + f32(ly3[sl, 0]) + f32(ly3[sl, 1])

        @pl.when(lax.rem(g, 2) == 0)
        def _():
            tq[c, :, pl.ds(0, ncu)] = bf(tu)
            tq[c, :, pl.ds(ncu, ncy)] = bf(ty)
            for k in range(2):
                fcopy(s, k).start()

        @pl.when(lax.rem(g, 2) == 1)
        def _():
            r = pl.ds(pl.multiple_of(e * re, 8), re)
            out[r, pl.ds(pl.multiple_of(role * half + cu, LANES), ncu)] = bf(tu)
            out[r, pl.ds(pl.multiple_of(role * half + cy, LANES), ncy)] = bf(ty)

    def reduce_step(i):
        @pl.when(i == 0)
        def _():
            sent(w.at[pl.ds(0, width), pl.ds(0, quarter)], drecv)
            load_w.wait()

        @pl.when(i == steps)
        def _():
            for k, (_, r, (_, c)) in enumerate(kinds):
                blocks = sum(kind(name) == kinds[k] for name in msgs) * r // rows
                sent(xl.at[OWN, pl.ds(0, blocks), :, pl.ds(0, c)], gsend.at[k])
            sent(w.at[pl.ds(0, width), pl.ds(0, quarter)], wsend)
            sent(w.at[pl.ds(0, width), pl.ds(0, quarter)], dsend)
            sent(hid.at[:, :, pl.ds(0, width)], hsend)

        for lag, stage in ((3 * LAG, stage4), (2 * LAG, stage3), (LAG, stage2), (0, stage1)):

            @pl.when((i >= lag) & (i < steps + lag))
            def _():
                stage(i - lag)

    reductions = [k for k, (_, kind) in enumerate(steps_) if kind == "B"]

    def body(j, _):
        communicate(j)
        before, here = jnp.int32(0), jnp.int32(0)
        for k in reductions:
            before += (j > k).astype(jnp.int32)
            here += (j == k).astype(jnp.int32)

        @pl.when(here == 0)
        def _():
            work(j - before)

        @pl.when(here == 1)
        def _():
            reduce_step(before)

        return 0

    lax.fori_loop(0, len(steps_) - 1, body, 0)
    for op in steps_[-1][0]:
        do(op)

    for e in range(EPOCHS):
        sent(out.at[pl.ds(0, re), pl.ds(0, half)], frecv.at[e])
    for s in (steps - 2, steps - 1):
        for k in (0, 2, 3, 5, 7, 8):
            left(s, k)
    for c in range(CHUNKS):
        sent(tq.at[c], fsend.at[c])


def solution(mesh):
    n = mesh.shape["tp"]

    def step(x, w_gate, w_up, w_down):
        (rows, depth), width = x.shape, w_gate.shape[1]
        order = plan(depth, rows, width)
        msgs = gather_messages(depth, rows)[0]
        re, half = rows // EPOCHS, depth // 2
        hr, unit = re // 2, depth // 28
        ncu, ncy = 8 * unit // CHUNKS, 6 * unit // CHUNKS
        pieces = half // 2 // 256
        tasks = 4 * EPOCHS
        pieces_of_sums = (2, 2, hr, ncu), (2, 2, re, ncu), (re, ncu), (4, re, ncy), (2, hr, ncy), (2, re, ncy)
        vmem = lambda *shape: pltpu.VMEM(shape, x.dtype)
        dma = lambda *shape: pltpu.SemaphoreType.DMA(shape)
        return pl.pallas_call(
            functools.partial(kernel, n, order, msgs),
            out_shape=(pltpu.VMEM(x.shape, x.dtype), jax.ShapeDtypeStruct((2, SLOTS, rows, depth), x.dtype)),
            in_specs=[pl.BlockSpec(memory_space=pl.ANY)] * 4,
            out_specs=(pl.BlockSpec(memory_space=pltpu.VMEM), pl.BlockSpec(memory_space=pl.ANY)),
            scratch_shapes=[
                vmem(3, depth, 2 * LANES),
                vmem(2 * width, half),
                vmem(2, 4 * re, depth),
                vmem(2 * EPOCHS * SLOTS, re, 2 * width),
                *(vmem(NB, *p) for p in pieces_of_sums),
                *(vmem(2, *p) for p in pieces_of_sums),
                vmem(CHUNKS, re, ncu + ncy),
                dma(len(send_kinds(msgs))),
                dma(len(msgs)),
                dma(2),
                dma(3),
                pltpu.SemaphoreType.DMA,
                pltpu.SemaphoreType.DMA,
                dma(pieces),
                pltpu.SemaphoreType.DMA,
                pltpu.SemaphoreType.DMA,
                pltpu.SemaphoreType.DMA,
                dma(tasks),
                dma(2, 6),
                dma(4, 10),
                dma(CHUNKS),
                dma(EPOCHS),
            ],
            compiler_params=pltpu.CompilerParams(
                collective_id=0, has_side_effects=True, vmem_limit_bytes=VLIM
            ),
        )(x, w_gate, w_up, w_down)[0]

    return jax.shard_map(
        step,
        mesh=mesh,
        in_specs=(P(("dp", "tp"), None), P(None, "tp"), P(None, "tp"), P("tp", None)),
        out_specs=P(("dp", "tp"), None),
        check_vma=False,
    )
```

```python
import functools
import math

import jax
import jax.numpy as jnp
from jax import lax
from jax.experimental import pallas as pl
from jax.experimental.pallas import tpu as pltpu
from jax.sharding import PartitionSpec as P

MESH = pl.DeviceIdType.MESH
LANES = 128
EPOCHS = 2
OWN, OTHER = 0, 1
TASK_SLOTS = ((0, 1, 2, 6), (3, 7, 4, 5))
GROUP_TILES = 3
LAG = 2
NB = 10
FLAGS = 6
CHUNKS = 4
BATCHES, STAGE_US = (range(3), range(3, 7), range(7, 10)), (1.62, 1.73, 1.2, 0.98)
VLIM = 64600000


FIRST_U, BY_PARTNER = (14, 17), 2
TUNE = {'due_w': (195, 100), 'due_f': (-1230, 1770), 'due_p': 3555, 'due_h': (-5230, -2790, 1010, 7030, 5030, 8890, 8690, 6690), 'backlog': 32, 'prefer': 26, 'phase': (0, 1.5, 3, 2.5)}


def columns(depth):
    t, (own, other) = depth // 28, FIRST_U
    end = 28 - BY_PARTNER
    return {
        OWN: ((0, own * t), (own * t, (28 - own) * t), None),
        OTHER: ((0, other * t), (other * t, (end - other) * t), (end * t, BY_PARTNER * t)),
    }


def gather_messages(depth, rows):
    msgs, deps = {}, {}
    re = rows // EPOCHS
    cols = columns(depth)

    def add(name, link, cls, src, dst, r, c, dep):
        msgs[name] = (link, cls, src, dst, r, c)
        deps[name] = dep

    for e in range(EPOCHS):
        every, a, b = (e * re, re), (e * re, re // 2), (e * re + re // 2, re // 2)
        add(("P1", OTHER, e), "P", OWN, 0, 0, every, cols[OTHER][0], [])
        add(("P2", OTHER, e), "P", OWN, 0, 0, every, (cols[OTHER][1][0], depth - cols[OTHER][1][0]), [])
        for cls in (OWN, OTHER):
            u, y, _ = cols[cls]
            m = lambda name: (name, cls, e)
            own_u = [] if cls == OWN else [("P1", OTHER, e)]
            own_y = [] if cls == OWN else [("P2", OTHER, e)]
            add(m("U1"), "U", cls, 0, 1, every, u, own_u)
            add(m("N1"), "N", cls, 0, 6, every, u, own_u)
            add(m("S1"), "S", cls, 0, 2, every, u, own_u)
            add(m("U2"), "U", cls, 0, 1, every, y, own_y)
            add(m("N2"), "N", cls, 0, 6, every, y, own_y)
            add(m("S2"), "S", cls, 0, 2, every, y, own_y)
            add(m("N3"), "N", cls, 1, 7, every, u, [m("U1")])
            add(m("S3"), "S", cls, 1, 3, every, u, [m("U1")])
            add(m("N4"), "N", cls, 6, 4, a, u, [m("N1")])
            add(m("S4"), "S", cls, 2, 4, b, u, [m("S1")])
            add(m("N5"), "N", cls, 6, 4, a, y, [m("N2")])
            add(m("S5"), "S", cls, 2, 4, b, y, [m("S2")])
            add(m("U3"), "U", cls, 6, 7, every, y, [m("N2")])
            add(m("U4"), "U", cls, 2, 3, every, y, [m("S2")])
            add(m("N6"), "N", cls, 7, 5, a, u, [m("N3")])
            add(m("S6"), "S", cls, 3, 5, b, u, [m("S3")])
            add(m("U5"), "U", cls, 4, 5, a, y, [m("N5")])
            add(m("U6"), "U", cls, 4, 5, b, y, [m("S5")])
        last = {1: ["U2"], 6: ["N2"], 2: ["S2"], 7: ["U3"], 3: ["U4"], 4: ["N5", "S5"], 5: ["U5", "U6"]}
        for s, need in last.items():
            add((f"F{s}", OTHER, e), "P", OWN, s, s, every, cols[OTHER][2], [(n, OWN, e) for n in need])
    return msgs, deps


def kind_of(message):
    to, cls, _, _, (_, r), cols = message
    return "P" if to == "P" else cls, r, cols


def send_kinds(msgs):
    return sorted({kind_of(m) for m in msgs.values()}, key=str)


def plan(depth, rows, width):
    rate, delay, tile_us, gt = 46.6e3, 2.3, 1.48, GROUP_TILES
    due_w, due_f, due_p, due_h, backlog = (TUNE[k] for k in ("due_w", "due_f", "due_p", "due_h", "backlog"))
    msgs, deps = gather_messages(depth, rows)
    pending = {name: set(d) for name, d in deps.items()}
    lack = {}
    for name, (link, cls, src, dst, r, c) in msgs.items():
        where = (OTHER if link == "P" else cls, name[2], dst)
        lack.setdefault(where, set()).add(name)
    pieces = depth // 4 // 256
    tasks = [(cls, e, h) for e in range(EPOCHS) for cls in (OWN, OTHER) for h in range(2)]
    subs = width // LANES // gt
    re, unit = rows // EPOCHS, depth // 28
    ncu, ncy = 8 * unit // CHUNKS, 6 * unit // CHUNKS
    nsteps = 2 * EPOCHS * CHUNKS
    copies = {}
    for i, (name, (link, cls, _, dst, (_, r), (_, c))) in enumerate(msgs.items()):
        e = name[2]
        if name[0][0] == "P":
            rank = due_p * e
        elif name[0][0] == "F":
            rank = due_f[e] + (15 if dst in TASK_SLOTS[1] else 0)
        else:
            rank = TUNE["phase"][2 * e + cls] * 1000 + i
        copies[name] = (link, r * c * 2, rank)
    for k in range(pieces):
        copies["W", k] = ("P", width * 256 * 2, due_w[0] + due_w[1] * k)
    for t in range(len(tasks)):
        copies["H", t] = ("P", 4 * re * width * 2, due_h[t] + 10 * t)
    u, y = re * ncu, re * ncy
    parts = (
        ("N", u), ("S", u), ("U", 4 * y), ("N", 2 * u), ("S", 2 * u), ("N", y // 2), ("S", y // 2), ("U", u), ("N", y), ("S", y),
    )
    free = dict.fromkeys("NSUPC", 0.0)
    avail = [n for n in msgs if not pending[n]] + [("W", k) for k in range(pieces)]
    now, arrivals = 0.0, []
    arrived = {}
    steps, ops = [], []
    loaded = {}
    task = sub = it = forwarded = 0

    def emit(*op):
        ops.append(op)

    def post(link, nbytes, what):
        free[link] = max(now, free[link]) + nbytes / (rate if link != "C" else 300e3)
        arrived[what] = free[link] + delay
        if what[0] not in "DHBE":
            arrivals.append((free[link] + delay, what))

    def issue():
        for n in sorted(avail, key=lambda n: copies[n][2]):
            link, nbytes, _ = copies[n]
            if free[link] - now < backlog:
                avail.remove(n)
                emit({"W": "wsend", "H": "hsend"}.get(n[0], "send"), n[1] if n[0] in "WH" else n)
                post(link, nbytes, n)
        for k in range(task, min(task + 2, len(tasks))):
            cls, e, h = tasks[k]
            for i, s in enumerate(TASK_SLOTS[h]):
                if (k, i) not in loaded and not lack.get((cls, e, s)):
                    loaded[k, i] = now + 1.5
                    emit("load", k, i)

    INF = 1e9

    def waits(j):
        return BATCHES[j - 1] if j else ()

    def active():
        return [(j, it - j * LAG) for j in range(4) if 0 <= it - j * LAG < nsteps]

    def b_ready():
        t, offset = 0.0, 0.0
        if it < nsteps and it % CHUNKS == 0:
            g = it // CHUNKS
            e, cls = g // 2, 1 - g % 2
            if task <= e * 4 + cls * 2 + 1 or forwarded < pieces:
                return INF
            t = max(arrived.get(("H", 2 * g + k), INF) for k in range(2))
            if it == 0:
                t = max(t, max(arrived["D", k] for k in range(pieces)))
        for j, s in active():
            t = max([t] + [arrived.get(("B", k, s), now + 5) - offset for k in waits(j)])
            offset += STAGE_US[j]
        return t

    while task < len(tasks) or it < nsteps + 3 * LAG:
        issue()
        for a in sorted((a for a in arrivals if a[0] <= now), key=lambda a: a[0]):
            arrivals.remove(a)
            what = a[1]
            now += 0.03
            emit("recv", what)
            if what[0] == "W":
                emit("forward", what[1])
                forwarded += 1
                post("C", width * 256 * 2, ("D", what[1]))
            else:
                for s in lack.values():
                    s.discard(what)
                for n in msgs:
                    if what in pending[n]:
                        pending[n].discard(what)
                        if not pending[n]:
                            avail.append(n)
            issue()
        tile_at = INF
        if task < len(tasks) and all((task, i) in loaded for i in range(4)):
            tile_at = max(loaded[task, i] for i in range(4))
        b_at = b_ready() if it < nsteps + 3 * LAG else INF
        choice = None
        if b_at <= now and tile_at <= now:
            choice = "B" if min(free["N"], free["U"]) - now < TUNE["prefer"] else "T"
        elif b_at <= now:
            choice = "B"
        elif tile_at <= now:
            choice = "T"
        if choice == "T":
            steps.append((ops, "T"))
            ops = []
            now += gt * tile_us
            sub += 1
            if sub == subs:
                avail.append(("H", task))
                task, sub = task + 1, 0
            continue
        if choice == "B":
            steps.append((ops, "B"))
            ops = []
            for j, s in active():
                now = max([now] + [arrived["B", k, s] for k in waits(j)]) + STAGE_US[j]
                for k in BATCHES[j] if j < len(BATCHES) else ():
                    link, n = parts[k]
                    post(link, 2 * n, ("B", k, s))
                if j == 3 and s // CHUNKS in (1, 2):
                    post("P", 2 * re * (ncu + ncy), ("E", s))
            now += 0.1
            it += 1
            continue
        times = [a[0] for a in arrivals] + [t for t in (tile_at, b_at) if now < t < INF]
        if avail:
            times.append(min(max(now + 0.3, free[copies[n][0]] - backlog + 0.1) for n in avail))
        now = max(now, min(times))
    assert not avail and not arrivals, (avail, arrivals)
    steps.append((ops, ""))
    return steps


def kernel(n, steps_, msgs, x_hbm, gate_hbm, up_hbm, down_hbm, out, xl, gbuf, w, xbuf, hid,
           lu1, lu2, lu3, ly1, ly2, ly3, tu1, tu2, tu3, ty1, ty2, ty3, tq,
           gsend, grecv, xsem, gusem, wosem, wsend, wrecv, dsend, drecv, hsend, hrecv,
           bsend, brecv, fsend, frecv):
    rows, depth = x_hbm.shape
    slots = n // 2
    width = gate_hbm.shape[1]
    re, half = rows // EPOCHS, depth // 2
    quarter, hr = half // 2, re // 2
    tiles = width // LANES
    pieces = quarter // 256
    unit = depth // 28
    ncu, ncy = 8 * unit // CHUNKS, 6 * unit // CHUNKS
    tasks = [(cls, e, h) for e in range(EPOCHS) for cls in (OWN, OTHER) for h in range(2)]
    total_tiles = len(tasks) * tiles
    steps = 2 * EPOCHS * CHUNKS

    side = math.isqrt(n)
    me, dp = lax.axis_index("tp"), lax.axis_index("dp")
    x, y = me // side, me % side
    role, core = ((x + 1) // 2) % 2, dp % 2
    link = {
        "N": {"tp": x * side + (y + 1) % side},
        "S": {"tp": x * side + (y + side - 1) % side},
        "U": {"tp": (side - 1 - x) * side + y},
        "P": {"tp": (x + 1 - 2 * (x % 2)) * side + y},
        "C": {"dp": dp + 1 - 2 * core},
    }

    def remote(src, dst, ssem, rsem, to):
        return pltpu.make_async_remote_copy(
            src_ref=src, dst_ref=dst, send_sem=ssem, recv_sem=rsem, device_id=link[to], device_id_type=MESH
        )

    def sent(ref, sem):
        pltpu.make_async_copy(ref, ref, sem).wait()

    def signal(sem, to):
        pl.semaphore_signal(sem, inc=1, device_id=link[to], device_id_type=MESH)

    barrier = pltpu.get_barrier_semaphore()
    for to in link:
        signal(barrier, to)

    index = {name: i for i, name in enumerate(msgs)}
    kinds = send_kinds(msgs)

    def kind(name):
        return kind_of(msgs[name])

    def source(cls, slot):
        return x_hbm if cls == OWN and slot == 0 else xl.at[cls, slot]

    def gcopy(name):
        to, cls, src, dst, (r, nr), (c, nc) = msgs[name]
        there = OTHER if to == "P" else cls
        block = (pl.ds(r, nr), pl.ds(c, nc))
        return remote(
            source(cls, src).at[block], xl.at[(there, dst, *block)], gsend.at[kinds.index(kind(name))], grecv.at[index[name]], to
        )

    def xload(t, i):
        cls, e, h = tasks[t]
        src = source(cls, TASK_SLOTS[h][i]).at[pl.ds(e * re, re)]
        return pltpu.make_async_copy(src, xbuf.at[t % 2, pl.ds(i * re, re)], xsem.at[t % 2])

    def load_tile(k):
        slot = lax.rem(k, 3)
        cols = pl.ds(pl.multiple_of(lax.rem(k, tiles) * LANES, LANES), LANES)
        return (
            pltpu.make_async_copy(gate_hbm.at[:, cols], gbuf.at[slot, :, pl.ds(0, LANES)], gusem.at[slot]),
            pltpu.make_async_copy(up_hbm.at[:, cols], gbuf.at[slot, :, pl.ds(LANES, LANES)], gusem.at[slot]),
        )

    def wcopy(k):
        there = pl.ds(pl.multiple_of(core * quarter + k * 256, LANES), 256)
        here = pl.ds(pl.multiple_of((1 - role) * half + core * quarter + k * 256, LANES), 256)
        return remote(down_hbm.at[:, here], w.at[pl.ds(width, width), there], wsend, wrecv.at[k], "P")

    def dcopy(k, whose):
        cols = pl.ds(pl.multiple_of(whose * quarter + k * 256, LANES), 256)
        block = w.at[pl.ds(width, width), cols]
        return remote(block, block, dsend, drecv, "C")

    def hcopy(t, i):
        cls, e, h = tasks[t]
        slot = TASK_SLOTS[h][i]
        src = hid.at[(2 * e + 1 - cls) * slots + slot, :, pl.ds(0, width)]
        dst = hid.at[(2 * e + cls) * slots + slot, :, pl.ds(width, width)]
        return remote(src, dst, hsend, hrecv.at[t], "P")

    def do(op):
        kind, what = op[0], op[1]
        if kind == "send":
            gcopy(what).start()
        elif kind == "recv" and what[0] == "W":
            wcopy(what[1]).wait_recv()
        elif kind == "recv":
            gcopy(what).wait_recv()
        elif kind == "load":
            xload(what, op[2]).start()
        elif kind == "wsend":
            wcopy(what).start()
        elif kind == "forward":
            dcopy(what, core).start()
        elif kind == "hsend":
            for i in range(4):
                hcopy(what, i).start()

    def communicate(j):
        for k, (ops, _) in enumerate(steps_):
            if ops:

                @pl.when(j == k)
                def _():
                    for op in ops:
                        do(op)

    def tile(k):
        t, i, slot = k // tiles, lax.rem(k, tiles), lax.rem(k, 3)
        cls, e, h = lax.rem(t // 2, 2), t // 4, lax.rem(t, 2)
        b = lax.rem(t, 2)

        @pl.when(i == 0)
        def _():
            sent(xbuf.at[b], xsem.at[b])

        sent(gbuf.at[slot], gusem.at[slot])

        @pl.when(k + 2 < total_tiles)
        def _():
            for c in load_tile(k + 2):
                c.start()

        acc = jnp.dot(xbuf[b], gbuf[slot], preferred_element_type=jnp.float32)
        gate, up = acc[:, :LANES], acc[:, LANES:]
        h_tile = (jax.nn.silu(gate) * up).astype(hid.dtype)
        cols = pl.ds(pl.multiple_of(i * LANES, LANES), LANES)
        for j in range(4):
            place = TASK_SLOTS[0][j] + h * (TASK_SLOTS[1][j] - TASK_SLOTS[0][j])
            hid[(2 * e + 1 - cls) * slots + place, :, cols] = h_tile[j * re : (j + 1) * re]

    def work(g):
        def one(i, _):
            tile(g * GROUP_TILES + i)
            return 0

        lax.fori_loop(0, GROUP_TILES, one, 0)

    pl.semaphore_wait(barrier, len(link))
    for c in load_tile(0) + load_tile(1):
        c.start()
    load_w = pltpu.make_async_copy(
        down_hbm.at[:, pl.ds(pl.multiple_of(role * half, LANES), half)], w.at[pl.ds(0, width)], wosem
    )
    load_w.start()

    def term(g, which, start, size):
        if which == tuple(range(which[0], which[0] + len(which))):
            lhs = hid[pl.ds(g * slots + which[0], len(which))].reshape(len(which) * re, 2 * width)
        else:
            lhs = jnp.concatenate([hid[g * slots + s] for s in which], axis=0)
        return jnp.dot(lhs, w[:, pl.ds(pl.multiple_of(start, LANES), size)], preferred_element_type=jnp.float32)

    f32 = lambda v: v.astype(jnp.float32)
    bf = lambda v: v.astype(jnp.bfloat16)

    def place(s):
        c = lax.rem(s, CHUNKS)
        return s // CHUNKS, c * ncu, 8 * unit + c * ncy, lax.rem(s, NB), lax.rem(s, 2)

    table = (
        ("N", tu1, 0, 0, lu1), ("S", tu1, 0, 1, lu1), ("U", ty1, 1, None, ly1),
        ("N", tu2, 2, 0, lu2), ("S", tu2, 2, 1, lu2), ("N", ty2, 3, 0, ly2), ("S", ty2, 3, 1, ly2),
        ("U", tu3, 4, None, lu3), ("N", ty3, 5, 0, ly3), ("S", ty3, 5, 1, ly3),
    )

    def bcopy(k, s):
        _, _, _, sl, st = place(s)
        to, staging, i, part, landing = table[k]
        src, dst = (staging.at[st], landing.at[sl]) if part is None else (staging.at[st, part], landing.at[sl, part])
        return remote(src, dst, bsend.at[st, i], brecv.at[lax.rem(s, FLAGS), table[k][2] // 2], to)

    def left(s, k):
        _, staging, i, _, _ = table[k]
        st = lax.rem(s, 2)
        sent(staging.at[st], bsend.at[st, i])

    def free_staging(s, copies):
        @pl.when(s >= 2)
        def _():
            for k in copies:
                left(s - 2, k)

    def arrived(s, batch):
        words = sum(math.prod(table[k][4].shape[1 if table[k][3] is None else 2 :]) for k in BATCHES[batch])
        sent(w.at[pl.ds(0, words // 256), pl.ds(0, 256)], brecv.at[lax.rem(s, FLAGS), batch])

    def stage1(s):
        g, cu, cy, sl, st = place(s)

        @pl.when(lax.rem(s, CHUNKS) == 0)
        def _():
            for h in range(2):
                sent(hid.at[pl.ds(g * slots, 4), :, pl.ds(width, width)], hrecv.at[2 * g + h])

        free_staging(s, (0, 2))
        t = term(g, (4, 5), cu, ncu).reshape(2, re, ncu)
        tu1[st, 0] = bf(t[:, :hr])
        tu1[st, 1] = bf(t[:, hr:])
        for k in (0, 1):
            bcopy(k, s).start()
        t = term(g, (1, 3, 5, 7), cy, ncy)
        ty1[st] = bf(t).reshape(4, re, ncy)
        bcopy(2, s).start()

    def stage2(s):
        g, cu, cy, sl, st = place(s)
        arrived(s, 0)
        free_staging(s, (3, 5))
        t = term(g, (2, 3), cu, ncu).reshape(2, re, ncu)
        tu2[st, 0, :, :hr] = bf(t[:, :hr] + f32(lu1[sl, 0]))
        tu2[st, 0, :, hr:] = bf(t[:, hr:])
        bcopy(3, s).start()
        t = term(g, (6, 7), cu, ncu).reshape(2, re, ncu)
        tu2[st, 1, :, :hr] = bf(t[:, :hr])
        tu2[st, 1, :, hr:] = bf(t[:, hr:] + f32(lu1[sl, 1]))
        bcopy(4, s).start()
        t = term(g, (4,), cy, ncy) + f32(ly1[sl, 2])
        ty2[st, 0] = bf(t[:hr])
        ty2[st, 1] = bf(t[hr:])
        for k in (5, 6):
            bcopy(k, s).start()

    def stage3(s):
        g, cu, cy, sl, st = place(s)
        arrived(s, 1)
        free_staging(s, (7, 8))
        t = term(g, (1,), cu, ncu)
        tu3[st] = bf(t + f32(lu2[sl, 0, 1]) + f32(lu2[sl, 1, 1]))
        bcopy(7, s).start()
        t = term(g, (2, 6), cy, ncy)
        a, b = t[:re] + f32(ly1[sl, 1]), t[re:] + f32(ly1[sl, 3])
        ty3[st, 0, :hr] = bf(a[:hr] + f32(ly2[sl, 0]))
        ty3[st, 0, hr:] = bf(a[hr:])
        ty3[st, 1, :hr] = bf(b[:hr])
        ty3[st, 1, hr:] = bf(b[hr:] + f32(ly2[sl, 1]))
        for k in (8, 9):
            bcopy(k, s).start()

    def fcopy(s, k):
        g, cu, cy, _, st = place(s)
        start, size = ((cu, ncu), (cy, ncy))[k]
        r = pl.ds(pl.multiple_of((g // 2) * re, 8), re)
        cols = pl.ds(pl.multiple_of(role * half + start, LANES), size)
        c = lax.rem(s, CHUNKS)
        return remote(tq.at[c, :, pl.ds(k * ncu, size)], out.at[r, cols], fsend.at[c], frecv.at[g // 2], "P")

    def stage4(s):
        g, cu, cy, sl, st = place(s)
        e, c = g // 2, lax.rem(s, CHUNKS)
        arrived(s, 2)

        @pl.when(lax.rem(g, 2) == 0)
        def _():
            @pl.when(e > 0)
            def _():
                sent(tq.at[c], fsend.at[c])

        tu = term(g, (0,), cu, ncu) + f32(lu2[sl, 0, 0]) + f32(lu2[sl, 1, 0]) + f32(lu3[sl])
        ty = term(g, (0,), cy, ncy) + f32(ly1[sl, 0]) + f32(ly3[sl, 0]) + f32(ly3[sl, 1])

        @pl.when(lax.rem(g, 2) == 0)
        def _():
            tq[c, :, pl.ds(0, ncu)] = bf(tu)
            tq[c, :, pl.ds(ncu, ncy)] = bf(ty)

        @pl.when((g == 1) | (g == 2))
        def _():
            for k in range(2):
                fcopy(s - CHUNKS * (2 - g), k).start()

        @pl.when(lax.rem(g, 2) == 1)
        def _():
            r = pl.ds(pl.multiple_of(e * re, 8), re)
            out[r, pl.ds(pl.multiple_of(role * half + cu, LANES), ncu)] = bf(tu)
            out[r, pl.ds(pl.multiple_of(role * half + cy, LANES), ncy)] = bf(ty)

    def reduce_step(i):
        @pl.when(i == 0)
        def _():
            sent(w.at[pl.ds(0, width), pl.ds(0, quarter)], drecv)
            load_w.wait()

        @pl.when(i == steps)
        def _():
            for k, (_, r, (_, c)) in enumerate(kinds):
                blocks = sum(kind(name) == kinds[k] for name in msgs) * r // rows
                sent(xl.at[OWN, pl.ds(0, blocks), :, pl.ds(0, c)], gsend.at[k])
            sent(w.at[pl.ds(0, width), pl.ds(0, quarter)], wsend)
            sent(w.at[pl.ds(0, width), pl.ds(0, quarter)], dsend)
            sent(hid.at[:, :, pl.ds(0, width)], hsend)

        for lag, stage in ((0, stage1), (LAG, stage2), (2 * LAG, stage3), (3 * LAG, stage4)):

            @pl.when((i >= lag) & (i < steps + lag))
            def _():
                stage(i - lag)

    reductions = [k for k, (_, kind) in enumerate(steps_) if kind == "B"]

    def body(j, _):
        communicate(j)
        before, here = jnp.int32(0), jnp.int32(0)
        for k in reductions:
            before += (j > k).astype(jnp.int32)
            here += (j == k).astype(jnp.int32)

        @pl.when(here == 0)
        def _():
            work(j - before)

        @pl.when(here == 1)
        def _():
            reduce_step(before)

        return 0

    lax.fori_loop(0, len(steps_) - 1, body, 0)
    for op in steps_[-1][0]:
        do(op)

    for e in range(EPOCHS):
        sent(out.at[pl.ds(0, re), pl.ds(0, half)], frecv.at[e])
    for s in (steps - 2, steps - 1):
        for k in (0, 2, 3, 5, 7, 8):
            left(s, k)
    for c in range(CHUNKS):
        sent(tq.at[c], fsend.at[c])


def solution(mesh):
    n = mesh.shape["tp"]

    def step(x, w_gate, w_up, w_down):
        (rows, depth), width = x.shape, w_gate.shape[1]
        order = plan(depth, rows, width)
        msgs = gather_messages(depth, rows)[0]
        re, half = rows // EPOCHS, depth // 2
        hr, unit = re // 2, depth // 28
        ncu, ncy = 8 * unit // CHUNKS, 6 * unit // CHUNKS
        pieces = half // 2 // 256
        tasks = 4 * EPOCHS
        pieces_of_sums = (2, 2, hr, ncu), (2, 2, re, ncu), (re, ncu), (4, re, ncy), (2, hr, ncy), (2, re, ncy)
        vmem = lambda *shape: pltpu.VMEM(shape, x.dtype)
        dma = lambda *shape: pltpu.SemaphoreType.DMA(shape)
        return pl.pallas_call(
            functools.partial(kernel, n, order, msgs),
            out_shape=(pltpu.VMEM(x.shape, x.dtype), jax.ShapeDtypeStruct((2, n // 2, rows, depth), x.dtype)),
            in_specs=[pl.BlockSpec(memory_space=pl.ANY)] * 4,
            out_specs=(pl.BlockSpec(memory_space=pltpu.VMEM), pl.BlockSpec(memory_space=pl.ANY)),
            scratch_shapes=[
                vmem(3, depth, 2 * LANES),
                vmem(2 * width, half),
                vmem(2, 4 * re, depth),
                vmem(EPOCHS * n, re, 2 * width),
                *(vmem(NB, *p) for p in pieces_of_sums),
                *(vmem(2, *p) for p in pieces_of_sums),
                vmem(CHUNKS, re, ncu + ncy),
                dma(len(send_kinds(msgs))),
                dma(len(msgs)),
                dma(2),
                dma(3),
                pltpu.SemaphoreType.DMA,
                pltpu.SemaphoreType.DMA,
                dma(pieces),
                pltpu.SemaphoreType.DMA,
                pltpu.SemaphoreType.DMA,
                pltpu.SemaphoreType.DMA,
                dma(tasks),
                dma(2, 6),
                dma(FLAGS, 3),
                dma(CHUNKS),
                dma(EPOCHS),
            ],
            compiler_params=pltpu.CompilerParams(
                collective_id=0, has_side_effects=True, vmem_limit_bytes=VLIM
            ),
        )(x, w_gate, w_up, w_down)[0]

    return jax.shard_map(
        step,
        mesh=mesh,
        in_specs=(P(("dp", "tp"), None), P(None, "tp"), P(None, "tp"), P("tp", None)),
        out_specs=P(("dp", "tp"), None),
        check_vma=False,
    )
```

```python
import functools
import math

import jax
import jax.numpy as jnp
from jax import lax
from jax.experimental import pallas as pl
from jax.experimental.pallas import tpu as pltpu
from jax.sharding import PartitionSpec as P

MESH = pl.DeviceIdType.MESH
LANES = 128
EPOCHS = 2
OWN, OTHER = 0, 1
TASK_SLOTS = (0, 1, 2, 6), (3, 7, 4, 5)
PARTS = ((1,), (2, 6), (0,)), ((3, 7, 4, 5),)
GROUP_TILES = 3
NB = 10
FLAGS = 7
CHUNKS = 4
LAGS = (0, 1, 3, 6), (0, 2, 4, 6)
STAGE_US = (0.6, 1.0, 0.57, 0.61), (0.98, 0.48, 0.61, 0.52)
LINKS = ("NS", "NS", "U"), ("U", "NS", "NS")
SHARE = (1, 2, 1), (4, 0.5, 1)
STAGES = [(i, j) for j in range(4) for i in range(2)]
VLIM = 64600000


FIRST_U, BY_PARTNER = (28, 31), 6
TUNE = {'due_w': (-2320, 691), 'due_f': (-3850, 1390), 'due_p': 1165, 'due_h': (-390, -1270, -4350, 1830, 870, 12450, 10410, 15370), 'backlog': 6, 'prefer': 48, 'phase': (1, 1, 3, 3), 'hb': 3110, 'blp': 10}


def columns(depth):
    t, (own, other) = depth // 56, FIRST_U
    end = 56 - BY_PARTNER
    return {
        OWN: ((0, own * t), (own * t, (56 - own) * t), None),
        OTHER: ((0, other * t), (other * t, (end - other) * t), (end * t, BY_PARTNER * t)),
    }


def gather_messages(depth, rows):
    msgs, deps = {}, {}
    re = rows // EPOCHS
    cols = columns(depth)

    def add(name, link, cls, src, dst, r, c, dep):
        msgs[name] = (link, cls, src, dst, r, c)
        deps[name] = dep

    for e in range(EPOCHS):
        every, a, b = (e * re, re), (e * re, re // 2), (e * re + re // 2, re // 2)
        add(("P1", OTHER, e), "P", OWN, 0, 0, every, cols[OTHER][0], [])
        add(("P2", OTHER, e), "P", OWN, 0, 0, every, (cols[OTHER][1][0], depth - cols[OTHER][1][0]), [])
        for cls in (OWN, OTHER):
            u, y, _ = cols[cls]
            m = lambda name: (name, cls, e)
            own_u = [] if cls == OWN else [("P1", OTHER, e)]
            own_y = [] if cls == OWN else [("P2", OTHER, e)]
            add(m("U1"), "U", cls, 0, 1, every, u, own_u)
            add(m("N1"), "N", cls, 0, 6, every, u, own_u)
            add(m("S1"), "S", cls, 0, 2, every, u, own_u)
            add(m("U2"), "U", cls, 0, 1, every, y, own_y)
            add(m("N2"), "N", cls, 0, 6, every, y, own_y)
            add(m("S2"), "S", cls, 0, 2, every, y, own_y)
            add(m("N3"), "N", cls, 1, 7, every, u, [m("U1")])
            add(m("S3"), "S", cls, 1, 3, every, u, [m("U1")])
            add(m("N4"), "N", cls, 6, 4, a, u, [m("N1")])
            add(m("S4"), "S", cls, 2, 4, b, u, [m("S1")])
            add(m("N5"), "N", cls, 6, 4, a, y, [m("N2")])
            add(m("S5"), "S", cls, 2, 4, b, y, [m("S2")])
            add(m("U3"), "U", cls, 6, 7, every, y, [m("N2")])
            add(m("U4"), "U", cls, 2, 3, every, y, [m("S2")])
            add(m("N6"), "N", cls, 7, 5, a, u, [m("N3")])
            add(m("S6"), "S", cls, 3, 5, b, u, [m("S3")])
            add(m("U5"), "U", cls, 4, 5, a, y, [m("N5")])
            add(m("U6"), "U", cls, 4, 5, b, y, [m("S5")])
        last = {1: ["U2"], 6: ["N2"], 2: ["S2"], 7: ["U3"], 3: ["U4"], 4: ["N5", "S5"], 5: ["U5", "U6"]}
        for s, need in last.items():
            add((f"F{s}", OTHER, e), "P", OWN, s, s, every, cols[OTHER][2], [(n, OWN, e) for n in need])
    return msgs, deps


def kind_of(message):
    to, cls, _, _, (_, r), cols = message
    return "P" if to == "P" else cls, r, cols


def send_kinds(msgs):
    return sorted({kind_of(m) for m in msgs.values()}, key=str)


def plan(depth, rows, width):
    rate, delay, tile_us, gt = 46.6e3, 2.3, 1.48, GROUP_TILES
    due_w, due_f, due_p, due_h, backlog = (TUNE[k] for k in ("due_w", "due_f", "due_p", "due_h", "backlog"))
    msgs, deps = gather_messages(depth, rows)
    pending = {name: set(d) for name, d in deps.items()}
    lack = {}
    for name, (link, cls, src, dst, r, c) in msgs.items():
        where = (OTHER if link == "P" else cls, name[2], dst)
        lack.setdefault(where, set()).add(name)
    pieces = depth // 4 // 256
    tasks = [(cls, e, h) for e in range(EPOCHS) for cls in (OWN, OTHER) for h in range(2)]
    subs = width // LANES // gt
    re, unit = rows // EPOCHS, depth // 28
    ncu, ncy = 8 * unit // CHUNKS, 6 * unit // CHUNKS
    nsteps = 2 * EPOCHS * CHUNKS
    copies = {}
    for i, (name, (link, cls, _, dst, (_, r), (_, c))) in enumerate(msgs.items()):
        e = name[2]
        if name[0][0] == "P":
            rank = due_p * e
        elif name[0][0] == "F":
            rank = due_f[e] + (15 if dst in TASK_SLOTS[1] else 0)
        else:
            rank = TUNE["phase"][2 * e + cls] * 1000 + i
        copies[name] = (link, r * c * 2, rank)
    for k in range(pieces):
        copies["W", k] = ("P", width * 256 * 2, due_w[0] + due_w[1] * k)
    for t in range(len(tasks)):
        for part, slots in enumerate(PARTS[t % 2]):
            due = due_h[t + 1] + 10 * t + 11 + part + TUNE["hb"] if part else due_h[t] + 10 * t
            copies["H", t, part] = ("P", len(slots) * re * width * 2, due)
    free = dict.fromkeys("NSUPC", 0.0)
    avail = [n for n in msgs if not pending[n]] + [("W", k) for k in range(pieces)]
    now, arrivals = 0.0, []
    arrived = {}
    steps, ops = [], []
    loaded = {}
    task = sub = it = forwarded = 0

    def emit(*op):
        ops.append(op)

    def post(link, nbytes, what):
        free[link] = max(now, free[link]) + nbytes / (rate if link != "C" else 300e3)
        arrived[what] = free[link] + delay
        if what[0] not in "DHBE":
            arrivals.append((free[link] + delay, what))

    def issue():
        for n in sorted(avail, key=lambda n: copies[n][2]):
            link, nbytes, _ = copies[n]
            if free[link] - now < (TUNE["blp"] if link == "P" else backlog):
                avail.remove(n)
                emit(*(("wsend", n[1]) if n[0] == "W" else ("hsend", *n[1:]) if n[0] == "H" else ("send", n)))
                post(link, nbytes, n)
        for k in range(task, min(task + 2, len(tasks))):
            cls, e, h = tasks[k]
            for i, s in enumerate(TASK_SLOTS[h]):
                if (k, i) not in loaded and not lack.get((cls, e, s)):
                    loaded[k, i] = now + 1.5
                    emit("load", k, i)

    INF = 1e9

    def active():
        return [(i, j, it - LAGS[i][j]) for i, j in STAGES if 0 <= it - LAGS[i][j] < nsteps]

    def waits(i, j):
        return [("B", i, j - 1, part) for part in range(len(LINKS[i][j - 1]))] if j else []

    def b_ready():
        t, offset = 0.0, 0.0
        if it < nsteps and it % CHUNKS == 0:
            g = it // CHUNKS
            e, cls = g // 2, 1 - g % 2
            if task <= e * 4 + cls * 2 + 1 or forwarded < pieces:
                return INF
            t = max(arrived.get(("H", 2 * g + k, 0), INF) for k in range(2))
            if it == 0:
                t = max(t, max(arrived["D", k] for k in range(pieces)))
        for i, j, s in active():
            t = max([t] + [arrived.get((*q, s), now + 5) - offset for q in waits(i, j)])
            offset += STAGE_US[i][j]
        return t

    while task < len(tasks) or it < nsteps + LAGS[1][3]:
        issue()
        for a in sorted((a for a in arrivals if a[0] <= now), key=lambda a: a[0]):
            arrivals.remove(a)
            what = a[1]
            now += 0.03
            emit("recv", what)
            if what[0] == "W":
                emit("forward", what[1])
                forwarded += 1
                post("C", width * 256 * 2, ("D", what[1]))
            else:
                for s in lack.values():
                    s.discard(what)
                for n in msgs:
                    if what in pending[n]:
                        pending[n].discard(what)
                        if not pending[n]:
                            avail.append(n)
            issue()
        tile_at = INF
        if task < len(tasks) and all((task, i) in loaded for i in range(4)):
            tile_at = max(loaded[task, i] for i in range(4))
        b_at = b_ready() if it < nsteps + LAGS[1][3] else INF
        choice = None
        if b_at <= now and tile_at <= now:
            choice = "B" if min(free["N"], free["U"]) - now < TUNE["prefer"] else "T"
        elif b_at <= now:
            choice = "B"
        elif tile_at <= now:
            choice = "T"
        if choice == "T":
            steps.append((ops, "T"))
            ops = []
            now += gt * tile_us
            sub += 1
            if sub == subs:
                avail.extend(("H", task, part) for part in range(len(PARTS[task % 2])))
                task, sub = task + 1, 0
            continue
        if choice == "B":
            steps.append((ops, "B"))
            ops = []
            for i, j, s in active():
                need = [(*q, s) for q in waits(i, j)]
                if s % CHUNKS == 0 and (i, j) in ((0, 1), (0, 3)):
                    need.append(("H", 2 * (s // CHUNKS), 1 if j == 1 else 2))
                now = max([now] + [arrived[q] for q in need]) + STAGE_US[i][j]
                for part, to in enumerate(LINKS[i][j] if j < 3 else ""):
                    post(to, 2 * SHARE[i][j] * re * (ncu, ncy)[i], ("B", i, j, part, s))
                if j == 3 and s // CHUNKS in (1, 2):
                    post("P", 2 * re * (ncu, ncy)[i], ("E", i, s))
            now += 0.3
            it += 1
            continue
        times = [a[0] for a in arrivals] + [t for t in (tile_at, b_at) if now < t < INF]
        if avail:
            times.append(min(max(now + 0.3, free[copies[n][0]] - (TUNE["blp"] if copies[n][0] == "P" else backlog) + 0.1) for n in avail))
        now = max(now, min(times))
    assert not avail and not arrivals, (avail, arrivals)
    steps.append((ops, ""))
    return steps


def kernel(n, steps_, msgs, x_hbm, gate_hbm, up_hbm, down_hbm, out, xl, gbuf, w, xbuf, hid,
           lu1, lu2, lu3, ly1, ly2, ly3, tu1, tu2, tu3, ty1, ty2, ty3, tq,
           gsend, grecv, xsem, gusem, wosem, wsend, wrecv, dsend, drecv, hsend, hrecv,
           bsend, brecv, fsend, frecv):
    rows, depth = x_hbm.shape
    slots = n // 2
    width = gate_hbm.shape[1]
    re, half = rows // EPOCHS, depth // 2
    quarter, hr = half // 2, re // 2
    tiles = width // LANES
    pieces = quarter // 256
    unit = depth // 28
    ncu, ncy = 8 * unit // CHUNKS, 6 * unit // CHUNKS
    tasks = [(cls, e, h) for e in range(EPOCHS) for cls in (OWN, OTHER) for h in range(2)]
    total_tiles = len(tasks) * tiles
    steps = 2 * EPOCHS * CHUNKS

    side = math.isqrt(n)
    me, dp = lax.axis_index("tp"), lax.axis_index("dp")
    x, y = me // side, me % side
    role, core = ((x + 1) // 2) % 2, dp % 2
    link = {
        "N": {"tp": x * side + (y + 1) % side},
        "S": {"tp": x * side + (y + side - 1) % side},
        "U": {"tp": (side - 1 - x) * side + y},
        "P": {"tp": (x + 1 - 2 * (x % 2)) * side + y},
        "C": {"dp": dp + 1 - 2 * core},
    }

    def remote(src, dst, ssem, rsem, to):
        return pltpu.make_async_remote_copy(
            src_ref=src, dst_ref=dst, send_sem=ssem, recv_sem=rsem, device_id=link[to], device_id_type=MESH
        )

    def sent(ref, sem):
        pltpu.make_async_copy(ref, ref, sem).wait()

    def signal(sem, to):
        pl.semaphore_signal(sem, inc=1, device_id=link[to], device_id_type=MESH)

    barrier = pltpu.get_barrier_semaphore()
    for to in link:
        signal(barrier, to)

    index = {name: i for i, name in enumerate(msgs)}
    kinds = send_kinds(msgs)

    def kind(name):
        return kind_of(msgs[name])

    def source(cls, slot):
        return x_hbm if cls == OWN and slot == 0 else xl.at[cls, slot]

    def gcopy(name):
        to, cls, src, dst, (r, nr), (c, nc) = msgs[name]
        there = OTHER if to == "P" else cls
        block = (pl.ds(r, nr), pl.ds(c, nc))
        return remote(
            source(cls, src).at[block], xl.at[(there, dst, *block)], gsend.at[kinds.index(kind(name))], grecv.at[index[name]], to
        )

    def xload(t, i):
        cls, e, h = tasks[t]
        src = source(cls, TASK_SLOTS[h][i]).at[pl.ds(e * re, re)]
        return pltpu.make_async_copy(src, xbuf.at[t % 2, pl.ds(i * re, re)], xsem.at[t % 2])

    def load_tile(k):
        slot = lax.rem(k, 3)
        cols = pl.ds(pl.multiple_of(lax.rem(k, tiles) * LANES, LANES), LANES)
        return (
            pltpu.make_async_copy(gate_hbm.at[:, cols], gbuf.at[slot, :, pl.ds(0, LANES)], gusem.at[slot]),
            pltpu.make_async_copy(up_hbm.at[:, cols], gbuf.at[slot, :, pl.ds(LANES, LANES)], gusem.at[slot]),
        )

    def wcopy(k):
        there = pl.ds(pl.multiple_of(core * quarter + k * 256, LANES), 256)
        here = pl.ds(pl.multiple_of((1 - role) * half + core * quarter + k * 256, LANES), 256)
        return remote(down_hbm.at[:, here], w.at[pl.ds(width, width), there], wsend, wrecv.at[k], "P")

    def dcopy(k, whose):
        cols = pl.ds(pl.multiple_of(whose * quarter + k * 256, LANES), 256)
        block = w.at[pl.ds(width, width), cols]
        return remote(block, block, dsend, drecv, "C")

    def hcopy(t, part, slot):
        cls, e, _ = tasks[t]
        src = hid.at[(2 * e + 1 - cls) * slots + slot, :, pl.ds(0, width)]
        dst = hid.at[(2 * e + cls) * slots + slot, :, pl.ds(width, width)]
        return remote(src, dst, hsend, hrecv.at[t, part], "P")

    def do(op):
        kind, what = op[0], op[1]
        if kind == "send":
            gcopy(what).start()
        elif kind == "recv" and what[0] == "W":
            wcopy(what[1]).wait_recv()
        elif kind == "recv":
            gcopy(what).wait_recv()
        elif kind == "load":
            xload(what, op[2]).start()
        elif kind == "wsend":
            wcopy(what).start()
        elif kind == "forward":
            dcopy(what, core).start()
        elif kind == "hsend":
            for slot in PARTS[what % 2][op[2]]:
                hcopy(what, op[2], slot).start()

    def communicate(j):
        for k, (ops, _) in enumerate(steps_):
            if ops:

                @pl.when(j == k)
                def _():
                    for op in ops:
                        do(op)

    def tile(k):
        t, i, slot = k // tiles, lax.rem(k, tiles), lax.rem(k, 3)
        cls, e, h = lax.rem(t // 2, 2), t // 4, lax.rem(t, 2)
        b = lax.rem(t, 2)

        @pl.when(i == 0)
        def _():
            sent(xbuf.at[b], xsem.at[b])

        sent(gbuf.at[slot], gusem.at[slot])

        @pl.when(k + 2 < total_tiles)
        def _():
            for c in load_tile(k + 2):
                c.start()

        acc = jnp.dot(xbuf[b], gbuf[slot], preferred_element_type=jnp.float32)
        gate, up = acc[:, :LANES], acc[:, LANES:]
        h_tile = (jax.nn.silu(gate) * up).astype(hid.dtype)
        cols = pl.ds(pl.multiple_of(i * LANES, LANES), LANES)
        for j in range(4):
            place = TASK_SLOTS[0][j] + h * (TASK_SLOTS[1][j] - TASK_SLOTS[0][j])
            hid[(2 * e + 1 - cls) * slots + place, :, cols] = h_tile[j * re : (j + 1) * re]

    def work(g):
        def one(i, _):
            tile(g * GROUP_TILES + i)
            return 0

        lax.fori_loop(0, GROUP_TILES, one, 0)

    pl.semaphore_wait(barrier, len(link))
    for c in load_tile(0) + load_tile(1):
        c.start()
    load_w = pltpu.make_async_copy(
        down_hbm.at[:, pl.ds(pl.multiple_of(role * half, LANES), half)], w.at[pl.ds(0, width)], wosem
    )
    load_w.start()

    def term(g, which, start, size):
        if which == tuple(range(which[0], which[0] + len(which))):
            lhs = hid[pl.ds(g * slots + which[0], len(which))].reshape(len(which) * re, 2 * width)
        else:
            lhs = jnp.concatenate([hid[g * slots + s] for s in which], axis=0)
        return jnp.dot(lhs, w[:, pl.ds(pl.multiple_of(start, LANES), size)], preferred_element_type=jnp.float32)

    f32 = lambda v: v.astype(jnp.float32)
    bf = lambda v: v.astype(jnp.bfloat16)

    def place(s):
        c = lax.rem(s, CHUNKS)
        return s // CHUNKS, c * ncu, 8 * unit + c * ncy, lax.rem(s, NB), lax.rem(s, 2)

    staging, landing = ((tu1, tu2, tu3), (ty1, ty2, ty3)), ((lu1, lu2, lu3), (ly1, ly2, ly3))

    def send(s, i, j):
        _, _, _, sl, st = place(s)
        for part, to in enumerate(LINKS[i][j]):
            src, dst = staging[i][j].at[st], landing[i][j].at[sl]
            if len(LINKS[i][j]) > 1:
                src, dst = src.at[part], dst.at[part]
            remote(src, dst, bsend.at[st, i, j], brecv.at[lax.rem(s, FLAGS), i, j], to).start()

    def left(s, i, j):
        st = lax.rem(s, 2)
        sent(staging[i][j].at[st], bsend.at[st, i, j])

    def free_staging(s, i, j):
        @pl.when(s >= 2)
        def _():
            left(s - 2, i, j)

    def arrived(s, i, j):
        _, _, _, sl, _ = place(s)
        sent(landing[i][j].at[sl], brecv.at[lax.rem(s, FLAGS), i, j])

    def partners(s, h, part):
        g = s // CHUNKS

        @pl.when(lax.rem(s, CHUNKS) == 0)
        def _():
            some = pl.ds(g * slots, len(PARTS[h][part]))
            sent(hid.at[some, :, pl.ds(width, width)], hrecv.at[2 * g + h, part])

    def u1(s):
        g, cu, cy, sl, st = place(s)

        partners(s, 0, 0)
        partners(s, 1, 0)
        free_staging(s, 0, 0)
        t = term(g, (4, 5), cu, ncu).reshape(2, re, ncu)
        tu1[st, 0] = bf(t[:, :hr])
        tu1[st, 1] = bf(t[:, hr:])
        send(s, 0, 0)

    def y1(s):
        g, cu, cy, sl, st = place(s)
        free_staging(s, 1, 0)
        ty1[st] = bf(term(g, (1, 3, 5, 7), cy, ncy)).reshape(4, re, ncy)
        send(s, 1, 0)

    def u2(s):
        g, cu, cy, sl, st = place(s)
        arrived(s, 0, 0)
        partners(s, 0, 1)
        free_staging(s, 0, 1)
        t = term(g, (2, 3), cu, ncu).reshape(2, re, ncu)
        tu2[st, 0, :, :hr] = bf(t[:, :hr] + f32(lu1[sl, 0]))
        tu2[st, 0, :, hr:] = bf(t[:, hr:])
        t = term(g, (6, 7), cu, ncu).reshape(2, re, ncu)
        tu2[st, 1, :, :hr] = bf(t[:, :hr])
        tu2[st, 1, :, hr:] = bf(t[:, hr:] + f32(lu1[sl, 1]))
        send(s, 0, 1)

    def y2(s):
        g, cu, cy, sl, st = place(s)
        arrived(s, 1, 0)
        free_staging(s, 1, 1)
        t = term(g, (4,), cy, ncy) + f32(ly1[sl, 2])
        ty2[st, 0] = bf(t[:hr])
        ty2[st, 1] = bf(t[hr:])
        send(s, 1, 1)

    def u3(s):
        g, cu, cy, sl, st = place(s)
        arrived(s, 0, 1)
        free_staging(s, 0, 2)
        tu3[st] = bf(term(g, (1,), cu, ncu) + f32(lu2[sl, 0, 1]) + f32(lu2[sl, 1, 1]))
        send(s, 0, 2)

    def y3(s):
        g, cu, cy, sl, st = place(s)
        arrived(s, 1, 1)
        free_staging(s, 1, 2)
        t = term(g, (2, 6), cy, ncy)
        a, b = t[:re] + f32(ly1[sl, 1]), t[re:] + f32(ly1[sl, 3])
        ty3[st, 0, :hr] = bf(a[:hr] + f32(ly2[sl, 0]))
        ty3[st, 0, hr:] = bf(a[hr:])
        ty3[st, 1, :hr] = bf(b[:hr])
        ty3[st, 1, hr:] = bf(b[hr:] + f32(ly2[sl, 1]))
        send(s, 1, 2)

    def u4(s):
        g, cu, cy, sl, st = place(s)
        arrived(s, 0, 2)
        partners(s, 0, 2)
        finish(s, 0, term(g, (0,), cu, ncu) + f32(lu2[sl, 0, 0]) + f32(lu2[sl, 1, 0]) + f32(lu3[sl]))

    def y4(s):
        g, cu, cy, sl, st = place(s)
        arrived(s, 1, 2)
        finish(s, 1, term(g, (0,), cy, ncy) + f32(ly1[sl, 0]) + f32(ly3[sl, 0]) + f32(ly3[sl, 1]))

    def fcopy(s, k):
        g, cu, cy, _, st = place(s)
        start, size = ((cu, ncu), (cy, ncy))[k]
        r = pl.ds(pl.multiple_of((g // 2) * re, 8), re)
        cols = pl.ds(pl.multiple_of(role * half + start, LANES), size)
        c = lax.rem(s, CHUNKS)
        return remote(tq.at[c, :, pl.ds(k * ncu, size)], out.at[r, cols], fsend.at[c, k], frecv.at[g // 2], "P")

    def finish(s, k, total):
        g, cu, cy, _, st = place(s)
        c = lax.rem(s, CHUNKS)
        start, size = ((cu, ncu), (cy, ncy))[k]
        piece = tq.at[c, :, pl.ds(k * ncu, size)]

        @pl.when(g == 2)
        def _():
            sent(piece, fsend.at[c, k])

        @pl.when(lax.rem(g, 2) == 0)
        def _():
            piece[...] = bf(total)

        @pl.when((g == 1) | (g == 2))
        def _():
            fcopy(s - CHUNKS * (2 - g), k).start()

        @pl.when(lax.rem(g, 2) == 1)
        def _():
            r = pl.ds(pl.multiple_of((g // 2) * re, 8), re)
            out[r, pl.ds(pl.multiple_of(role * half + start, LANES), size)] = bf(total)

    def reduce_step(i):
        @pl.when(i == 0)
        def _():
            sent(w.at[pl.ds(0, width), pl.ds(0, quarter)], drecv)
            load_w.wait()

        @pl.when(i == steps)
        def _():
            for k, (_, r, (_, c)) in enumerate(kinds):
                blocks = sum(kind(name) == kinds[k] for name in msgs) * r // rows
                sent(xl.at[OWN, pl.ds(0, blocks), :, pl.ds(0, c)], gsend.at[k])
            sent(w.at[pl.ds(0, width), pl.ds(0, quarter)], wsend)
            sent(w.at[pl.ds(0, width), pl.ds(0, quarter)], dsend)
            sent(hid.at[:, :, pl.ds(0, width)], hsend)

        for (a, b), stage in zip(STAGES, (u1, y1, u2, y2, u3, y3, u4, y4), strict=True):
            lag = LAGS[a][b]

            @pl.when((i >= lag) & (i < steps + lag))
            def _():
                stage(i - lag)

    reductions = [k for k, (_, kind) in enumerate(steps_) if kind == "B"]

    def body(j, _):
        communicate(j)
        before, here = jnp.int32(0), jnp.int32(0)
        for k in reductions:
            before += (j > k).astype(jnp.int32)
            here += (j == k).astype(jnp.int32)

        @pl.when(here == 0)
        def _():
            work(j - before)

        @pl.when(here == 1)
        def _():
            reduce_step(before)

        return 0

    lax.fori_loop(0, len(steps_) - 1, body, 0)
    for op in steps_[-1][0]:
        do(op)

    for e in range(EPOCHS):
        sent(out.at[pl.ds(0, re), pl.ds(0, half)], frecv.at[e])
    for s in (steps - 2, steps - 1):
        for i, j in STAGES[:-2]:
            left(s, i, j)
    for c in range(CHUNKS):
        for k in range(2):
            sent(tq.at[c, :, pl.ds(k * ncu, (ncu, ncy)[k])], fsend.at[c, k])


def solution(mesh):
    n = mesh.shape["tp"]

    def step(x, w_gate, w_up, w_down):
        (rows, depth), width = x.shape, w_gate.shape[1]
        order = plan(depth, rows, width)
        msgs = gather_messages(depth, rows)[0]
        re, half = rows // EPOCHS, depth // 2
        hr, unit = re // 2, depth // 28
        ncu, ncy = 8 * unit // CHUNKS, 6 * unit // CHUNKS
        pieces = half // 2 // 256
        tasks = 4 * EPOCHS
        pieces_of_sums = (2, 2, hr, ncu), (2, 2, re, ncu), (re, ncu), (4, re, ncy), (2, hr, ncy), (2, re, ncy)
        vmem = lambda *shape: pltpu.VMEM(shape, x.dtype)
        dma = lambda *shape: pltpu.SemaphoreType.DMA(shape)
        return pl.pallas_call(
            functools.partial(kernel, n, order, msgs),
            out_shape=(pltpu.VMEM(x.shape, x.dtype), jax.ShapeDtypeStruct((2, n // 2, rows, depth), x.dtype)),
            in_specs=[pl.BlockSpec(memory_space=pl.ANY)] * 4,
            out_specs=(pl.BlockSpec(memory_space=pltpu.VMEM), pl.BlockSpec(memory_space=pl.ANY)),
            scratch_shapes=[
                vmem(3, depth, 2 * LANES),
                vmem(2 * width, half),
                vmem(2, 4 * re, depth),
                vmem(EPOCHS * n, re, 2 * width),
                *(vmem(NB, *p) for p in pieces_of_sums),
                *(vmem(2, *p) for p in pieces_of_sums),
                vmem(CHUNKS, re, ncu + ncy),
                dma(len(send_kinds(msgs))),
                dma(len(msgs)),
                dma(2),
                dma(3),
                pltpu.SemaphoreType.DMA,
                pltpu.SemaphoreType.DMA,
                dma(pieces),
                pltpu.SemaphoreType.DMA,
                pltpu.SemaphoreType.DMA,
                pltpu.SemaphoreType.DMA,
                dma(tasks, 3),
                dma(2, 2, 3),
                dma(FLAGS, 2, 3),
                dma(CHUNKS, 2),
                dma(EPOCHS),
            ],
            compiler_params=pltpu.CompilerParams(
                collective_id=0, has_side_effects=True, vmem_limit_bytes=VLIM
            ),
        )(x, w_gate, w_up, w_down)[0]

    return jax.shard_map(
        step,
        mesh=mesh,
        in_specs=(P(("dp", "tp"), None), P(None, "tp"), P(None, "tp"), P("tp", None)),
        out_specs=P(("dp", "tp"), None),
        check_vma=False,
    )
```

```python
import functools
import math

import jax
import jax.numpy as jnp
from jax import lax
from jax.experimental import pallas as pl
from jax.experimental.pallas import tpu as pltpu
from jax.sharding import PartitionSpec as P

MESH = pl.DeviceIdType.MESH
LANES = 128
EPOCHS = 2
OWN, OTHER = 0, 1
TASK_SLOTS = (0, 1, 2, 6), (3, 7, 4, 5)
PARTS = ((1,), (2, 6), (0,)), ((3, 7, 4, 5),)
GROUP_TILES = 3
NB = 10
FLAGS = 7
CHUNKS = 4
LAGS = (0, 1, 3, 6), (0, 2, 4, 6)
STAGE_US = (0.6, 1.0, 0.57, 0.61), (0.98, 0.48, 0.61, 0.52)
LINKS = ("NS", "NS", "U"), ("U", "NS", "NS")
SHARE = (1, 2, 1), (4, 0.5, 1)
STAGES = [(i, j) for j in range(4) for i in range(2)]
VLIM = 64600000


FIRST_U, BY_PARTNER = (30, 29), 6
TUNE = {'due_w': (-2685, 675), 'due_f': (-5900, 2080), 'due_p': 1315, 'due_h': (270, 590, 1590, 7110, 5130, 13430, 15010, 26350), 'backlog': 11, 'prefer': 24, 'phase': (0, 0, 2, 1.5), 'hb': 1190, 'blp': 10}


def columns(depth):
    t, (own, other) = depth // 56, FIRST_U
    end = 56 - BY_PARTNER
    return {
        OWN: ((0, own * t), (own * t, (56 - own) * t), None),
        OTHER: ((0, other * t), (other * t, (end - other) * t), (end * t, BY_PARTNER * t)),
    }


def gather_messages(depth, rows):
    msgs, deps = {}, {}
    re = rows // EPOCHS
    cols = columns(depth)

    def add(name, link, cls, src, dst, r, c, dep):
        msgs[name] = (link, cls, src, dst, r, c)
        deps[name] = dep

    for e in range(EPOCHS):
        every, a, b = (e * re, re), (e * re, re // 2), (e * re + re // 2, re // 2)
        add(("P1", OTHER, e), "P", OWN, 0, 0, every, cols[OTHER][0], [])
        add(("P2", OTHER, e), "P", OWN, 0, 0, every, (cols[OTHER][1][0], depth - cols[OTHER][1][0]), [])
        for cls in (OWN, OTHER):
            u, y, _ = cols[cls]
            m = lambda name: (name, cls, e)
            own_u = [] if cls == OWN else [("P1", OTHER, e)]
            own_y = [] if cls == OWN else [("P2", OTHER, e)]
            add(m("U1"), "U", cls, 0, 1, every, u, own_u)
            add(m("N1"), "N", cls, 0, 6, every, u, own_u)
            add(m("S1"), "S", cls, 0, 2, every, u, own_u)
            add(m("U2"), "U", cls, 0, 1, every, y, own_y)
            add(m("N2"), "N", cls, 0, 6, every, y, own_y)
            add(m("S2"), "S", cls, 0, 2, every, y, own_y)
            add(m("N3"), "N", cls, 1, 7, every, u, [m("U1")])
            add(m("S3"), "S", cls, 1, 3, every, u, [m("U1")])
            add(m("N4"), "N", cls, 6, 4, a, u, [m("N1")])
            add(m("S4"), "S", cls, 2, 4, b, u, [m("S1")])
            add(m("N5"), "N", cls, 6, 4, a, y, [m("N2")])
            add(m("S5"), "S", cls, 2, 4, b, y, [m("S2")])
            add(m("U3"), "U", cls, 6, 7, every, y, [m("N2")])
            add(m("U4"), "U", cls, 2, 3, every, y, [m("S2")])
            add(m("N6"), "N", cls, 7, 5, a, u, [m("N3")])
            add(m("S6"), "S", cls, 3, 5, b, u, [m("S3")])
            add(m("U5"), "U", cls, 4, 5, a, y, [m("N5")])
            add(m("U6"), "U", cls, 4, 5, b, y, [m("S5")])
        last = {1: ["U2"], 6: ["N2"], 2: ["S2"], 7: ["U3"], 3: ["U4"], 4: ["N5", "S5"], 5: ["U5", "U6"]}
        for s, need in last.items():
            add((f"F{s}", OTHER, e), "P", OWN, s, s, every, cols[OTHER][2], [(n, OWN, e) for n in need])
    return msgs, deps


def kind_of(message):
    to, cls, _, _, (_, r), cols = message
    return "P" if to == "P" else cls, r, cols


def send_kinds(msgs):
    return sorted({kind_of(m) for m in msgs.values()}, key=str)


def arrivals_of(msgs, deps):
    handed_on = set().union(*deps.values())
    key = {m: m if m in handed_on else (OTHER if v[0] == "P" else v[1], m[2], v[3]) for m, v in msgs.items()}
    order = {k: i for i, k in enumerate(dict.fromkeys(key.values()))}
    return key, order


def plan(depth, rows, width):
    rate, delay, tile_us, gt = 46.6e3, 2.3, 1.48, GROUP_TILES
    due_w, due_f, due_p, due_h, backlog = (TUNE[k] for k in ("due_w", "due_f", "due_p", "due_h", "backlog"))
    msgs, deps = gather_messages(depth, rows)
    pending = {name: set(d) for name, d in deps.items()}
    lack = {}
    for name, (link, cls, src, dst, r, c) in msgs.items():
        where = (OTHER if link == "P" else cls, name[2], dst)
        lack.setdefault(where, set()).add(name)
    pieces = depth // 4 // 256
    tasks = [(cls, e, h) for e in range(EPOCHS) for cls in (OWN, OTHER) for h in range(2)]
    subs = width // LANES // gt
    re, unit = rows // EPOCHS, depth // 28
    ncu, ncy = 8 * unit // CHUNKS, 6 * unit // CHUNKS
    nsteps = 2 * EPOCHS * CHUNKS
    copies = {}
    for i, (name, (link, cls, _, dst, (_, r), (_, c))) in enumerate(msgs.items()):
        e = name[2]
        if name[0][0] == "P":
            rank = due_p * e
        elif name[0][0] == "F":
            rank = due_f[e] + (15 if dst in TASK_SLOTS[1] else 0)
        else:
            rank = TUNE["phase"][2 * e + cls] * 1000 + i
        copies[name] = (link, r * c * 2, rank)
    for k in range(pieces):
        copies["W", k] = ("P", width * 256 * 2, due_w[0] + due_w[1] * k)
    for t in range(len(tasks)):
        for part, slots in enumerate(PARTS[t % 2]):
            due = due_h[t + 1] + 10 * t + 11 + part + TUNE["hb"] if part else due_h[t] + 10 * t
            copies["H", t, part] = ("P", len(slots) * re * width * 2, due)
    free = dict.fromkeys("NSUPC", 0.0)
    avail = [n for n in msgs if not pending[n]] + [("W", k) for k in range(pieces)]
    now, arrivals = 0.0, []
    arrived = {}
    steps, ops = [], []
    loaded = {}
    task = sub = it = forwarded = 0

    def emit(*op):
        ops.append(op)

    def post(link, nbytes, what):
        free[link] = max(now, free[link]) + nbytes / (rate if link != "C" else 300e3)
        arrived[what] = free[link] + delay
        if what[0] not in "DHBE":
            arrivals.append((free[link] + delay, what))

    def issue():
        for n in sorted(avail, key=lambda n: copies[n][2]):
            link, nbytes, _ = copies[n]
            if free[link] - now < (TUNE["blp"] if link == "P" else backlog):
                avail.remove(n)
                emit(*(("wsend", n[1]) if n[0] == "W" else ("hsend", *n[1:]) if n[0] == "H" else ("send", n)))
                post(link, nbytes, n)
        for k in range(task, min(task + 2, len(tasks))):
            cls, e, h = tasks[k]
            for i, s in enumerate(TASK_SLOTS[h]):
                if (k, i) not in loaded and not lack.get((cls, e, s)):
                    loaded[k, i] = now + 1.5
                    emit("load", k, i)

    INF = 1e9

    def active():
        return [(i, j, it - LAGS[i][j]) for i, j in STAGES if 0 <= it - LAGS[i][j] < nsteps]

    def waits(i, j):
        return [("B", i, j - 1, part) for part in range(len(LINKS[i][j - 1]))] if j else []

    def b_ready():
        t, offset = 0.0, 0.0
        if it < nsteps and it % CHUNKS == 0:
            g = it // CHUNKS
            e, cls = g // 2, 1 - g % 2
            if task <= e * 4 + cls * 2 + 1 or forwarded < pieces:
                return INF
            t = max(arrived.get(("H", 2 * g + k, 0), INF) for k in range(2))
            if it == 0:
                t = max(t, max(arrived["D", k] for k in range(pieces)))
        for i, j, s in active():
            t = max([t] + [arrived.get((*q, s), now + 5) - offset for q in waits(i, j)])
            offset += STAGE_US[i][j]
        return t

    while task < len(tasks) or it < nsteps + LAGS[1][3]:
        issue()
        for a in sorted((a for a in arrivals if a[0] <= now), key=lambda a: a[0]):
            arrivals.remove(a)
            what = a[1]
            now += 0.03
            emit("recv", what)
            if what[0] == "W":
                emit("forward", what[1])
                forwarded += 1
                post("C", width * 256 * 2, ("D", what[1]))
            else:
                for s in lack.values():
                    s.discard(what)
                for n in msgs:
                    if what in pending[n]:
                        pending[n].discard(what)
                        if not pending[n]:
                            avail.append(n)
            issue()
        tile_at = INF
        if task < len(tasks) and all((task, i) in loaded for i in range(4)):
            tile_at = max(loaded[task, i] for i in range(4))
        b_at = b_ready() if it < nsteps + LAGS[1][3] else INF
        choice = None
        if b_at <= now and tile_at <= now:
            choice = "B" if min(free["N"], free["U"]) - now < TUNE["prefer"] else "T"
        elif b_at <= now:
            choice = "B"
        elif tile_at <= now:
            choice = "T"
        if choice == "T":
            steps.append((ops, "T"))
            ops = []
            now += gt * tile_us
            sub += 1
            if sub == subs:
                avail.extend(("H", task, part) for part in range(len(PARTS[task % 2])))
                task, sub = task + 1, 0
            continue
        if choice == "B":
            steps.append((ops, "B"))
            ops = []
            for i, j, s in active():
                need = [(*q, s) for q in waits(i, j)]
                if s % CHUNKS == 0 and (i, j) in ((0, 1), (0, 3)):
                    need.append(("H", 2 * (s // CHUNKS), 1 if j == 1 else 2))
                now = max([now] + [arrived[q] for q in need]) + STAGE_US[i][j]
                for part, to in enumerate(LINKS[i][j] if j < 3 else ""):
                    post(to, 2 * SHARE[i][j] * re * (ncu, ncy)[i], ("B", i, j, part, s))
                if j == 3 and s // CHUNKS in (1, 2):
                    post("P", 2 * re * (ncu, ncy)[i], ("E", i, s))
            now += 0.3
            it += 1
            continue
        times = [a[0] for a in arrivals] + [t for t in (tile_at, b_at) if now < t < INF]
        if avail:
            times.append(min(max(now + 0.3, free[copies[n][0]] - (TUNE["blp"] if copies[n][0] == "P" else backlog) + 0.1) for n in avail))
        now = max(now, min(times))
    assert not avail and not arrivals, (avail, arrivals)
    steps.append((ops, ""))
    return steps


def kernel(n, steps_, msgs, x_hbm, gate_hbm, up_hbm, down_hbm, out, xl, gbuf, w, xbuf, hid,
           lu1, lu2, lu3, ly1, ly2, ly3, tu1, tu2, tu3, ty1, ty2, ty3, tq,
           gsend, grecv, xsem, gusem, wosem, wsend, wrecv, dsend, drecv, hsend, hrecv,
           bsend, brecv, fsend, frecv):
    rows, depth = x_hbm.shape
    slots = n // 2
    width = gate_hbm.shape[1]
    re, half = rows // EPOCHS, depth // 2
    quarter, hr = half // 2, re // 2
    tiles = width // LANES
    pieces = quarter // 256
    unit = depth // 28
    ncu, ncy = 8 * unit // CHUNKS, 6 * unit // CHUNKS
    tasks = [(cls, e, h) for e in range(EPOCHS) for cls in (OWN, OTHER) for h in range(2)]
    total_tiles = len(tasks) * tiles
    steps = 2 * EPOCHS * CHUNKS

    side = math.isqrt(n)
    me, dp = lax.axis_index("tp"), lax.axis_index("dp")
    x, y = me // side, me % side
    role, core = ((x + 1) // 2) % 2, dp % 2
    link = {
        "N": {"tp": x * side + (y + 1) % side},
        "S": {"tp": x * side + (y + side - 1) % side},
        "U": {"tp": (side - 1 - x) * side + y},
        "P": {"tp": (x + 1 - 2 * (x % 2)) * side + y},
        "C": {"dp": dp + 1 - 2 * core},
    }

    def remote(src, dst, ssem, rsem, to):
        return pltpu.make_async_remote_copy(
            src_ref=src, dst_ref=dst, send_sem=ssem, recv_sem=rsem, device_id=link[to], device_id_type=MESH
        )

    def sent(ref, sem):
        pltpu.make_async_copy(ref, ref, sem).wait()

    def signal(sem, to):
        pl.semaphore_signal(sem, inc=1, device_id=link[to], device_id_type=MESH)

    barrier = pltpu.get_barrier_semaphore()
    for to in link:
        signal(barrier, to)

    key, arrival = arrivals_of(msgs, gather_messages(depth, rows)[1])
    kinds = send_kinds(msgs)

    def kind(name):
        return kind_of(msgs[name])

    def source(cls, slot):
        return x_hbm if cls == OWN and slot == 0 else xl.at[cls, slot]

    def gcopy(name):
        to, cls, src, dst, (r, nr), (c, nc) = msgs[name]
        there = OTHER if to == "P" else cls
        block = (pl.ds(r, nr), pl.ds(c, nc))
        return remote(
            source(cls, src).at[block], xl.at[(there, dst, *block)], gsend.at[kinds.index(kind(name))], grecv.at[arrival[key[name]]], to
        )

    def xload(t, i):
        cls, e, h = tasks[t]
        src = source(cls, TASK_SLOTS[h][i]).at[pl.ds(e * re, re)]
        return pltpu.make_async_copy(src, xbuf.at[t % 2, pl.ds(i * re, re)], xsem.at[t % 2])

    def load_tile(k):
        slot = lax.rem(k, 3)
        cols = pl.ds(pl.multiple_of(lax.rem(k, tiles) * LANES, LANES), LANES)
        return (
            pltpu.make_async_copy(gate_hbm.at[:, cols], gbuf.at[slot, :, pl.ds(0, LANES)], gusem.at[slot]),
            pltpu.make_async_copy(up_hbm.at[:, cols], gbuf.at[slot, :, pl.ds(LANES, LANES)], gusem.at[slot]),
        )

    def wcopy(k):
        there = pl.ds(pl.multiple_of(core * quarter + k * 256, LANES), 256)
        here = pl.ds(pl.multiple_of((1 - role) * half + core * quarter + k * 256, LANES), 256)
        return remote(down_hbm.at[:, here], w.at[pl.ds(width, width), there], wsend, wrecv.at[k], "P")

    def dcopy(k, whose):
        cols = pl.ds(pl.multiple_of(whose * quarter + k * 256, LANES), 256)
        block = w.at[pl.ds(width, width), cols]
        return remote(block, block, dsend, drecv, "C")

    def hcopy(t, part, slot):
        cls, e, _ = tasks[t]
        src = hid.at[(2 * e + 1 - cls) * slots + slot, :, pl.ds(0, width)]
        dst = hid.at[(2 * e + cls) * slots + slot, :, pl.ds(width, width)]
        return remote(src, dst, hsend, hrecv.at[t, part], "P")

    def do(op):
        kind, what = op[0], op[1]
        if kind == "send":
            gcopy(what).start()
        elif kind == "recv" and what[0] == "W":
            wcopy(what[1]).wait_recv()
        elif kind == "recv":
            if key[what] == what:
                gcopy(what).wait_recv()
        elif kind == "load":
            cls, e, h = tasks[what]
            slot = TASK_SLOTS[h][op[2]]
            rest = sum(math.prod(b for _, b in m[4:]) for name, m in msgs.items() if key[name] == (cls, e, slot))
            if rest:
                filled = xl.at[cls, slot, pl.ds(e * re, re), pl.ds(0, rest // re)]
                sent(filled, grecv.at[arrival[cls, e, slot]])
            xload(what, op[2]).start()
        elif kind == "wsend":
            wcopy(what).start()
        elif kind == "forward":
            dcopy(what, core).start()
        elif kind == "hsend":
            for slot in PARTS[what % 2][op[2]]:
                hcopy(what, op[2], slot).start()

    def communicate(j):
        for k, (ops, _) in enumerate(steps_):
            if ops:

                @pl.when(j == k)
                def _():
                    for op in ops:
                        do(op)

    def tile(k):
        t, i, slot = k // tiles, lax.rem(k, tiles), lax.rem(k, 3)
        cls, e, h = lax.rem(t // 2, 2), t // 4, lax.rem(t, 2)
        b = lax.rem(t, 2)

        @pl.when(i == 0)
        def _():
            sent(xbuf.at[b], xsem.at[b])

        sent(gbuf.at[slot], gusem.at[slot])

        @pl.when(k + 2 < total_tiles)
        def _():
            for c in load_tile(k + 2):
                c.start()

        acc = jnp.dot(xbuf[b], gbuf[slot], preferred_element_type=jnp.float32)
        gate, up = acc[:, :LANES], acc[:, LANES:]
        h_tile = (jax.nn.silu(gate) * up).astype(hid.dtype)
        cols = pl.ds(pl.multiple_of(i * LANES, LANES), LANES)
        for j in range(4):
            place = TASK_SLOTS[0][j] + h * (TASK_SLOTS[1][j] - TASK_SLOTS[0][j])
            hid[(2 * e + 1 - cls) * slots + place, :, cols] = h_tile[j * re : (j + 1) * re]

    def work(g):
        def one(i, _):
            tile(g * GROUP_TILES + i)
            return 0

        lax.fori_loop(0, GROUP_TILES, one, 0)

    pl.semaphore_wait(barrier, len(link))
    for c in load_tile(0) + load_tile(1):
        c.start()
    load_w = pltpu.make_async_copy(
        down_hbm.at[:, pl.ds(pl.multiple_of(role * half, LANES), half)], w.at[pl.ds(0, width)], wosem
    )
    load_w.start()

    def term(g, which, start, size):
        if which == tuple(range(which[0], which[0] + len(which))):
            lhs = hid[pl.ds(g * slots + which[0], len(which))].reshape(len(which) * re, 2 * width)
        else:
            lhs = jnp.concatenate([hid[g * slots + s] for s in which], axis=0)
        return jnp.dot(lhs, w[:, pl.ds(pl.multiple_of(start, LANES), size)], preferred_element_type=jnp.float32)

    f32 = lambda v: v.astype(jnp.float32)
    bf = lambda v: v.astype(jnp.bfloat16)

    def place(s):
        c = lax.rem(s, CHUNKS)
        return s // CHUNKS, c * ncu, 8 * unit + c * ncy, lax.rem(s, NB), lax.rem(s, 2)

    staging, landing = ((tu1, tu2, tu3), (ty1, ty2, ty3)), ((lu1, lu2, lu3), (ly1, ly2, ly3))

    def send(s, i, j):
        _, _, _, sl, st = place(s)
        for part, to in enumerate(LINKS[i][j]):
            src, dst = staging[i][j].at[st], landing[i][j].at[sl]
            if len(LINKS[i][j]) > 1:
                src, dst = src.at[part], dst.at[part]
            remote(src, dst, bsend.at[st, i, j], brecv.at[lax.rem(s, FLAGS), i, j], to).start()

    def left(s, i, j):
        st = lax.rem(s, 2)
        sent(staging[i][j].at[st], bsend.at[st, i, j])

    def free_staging(s, i, j):
        @pl.when(s >= 2)
        def _():
            left(s - 2, i, j)

    def arrived(s, i, j):
        _, _, _, sl, _ = place(s)
        sent(landing[i][j].at[sl], brecv.at[lax.rem(s, FLAGS), i, j])

    def partners(s, h, part):
        g = s // CHUNKS

        @pl.when(lax.rem(s, CHUNKS) == 0)
        def _():
            some = pl.ds(g * slots, len(PARTS[h][part]))
            sent(hid.at[some, :, pl.ds(width, width)], hrecv.at[2 * g + h, part])

    def u1(s):
        g, cu, cy, sl, st = place(s)

        partners(s, 0, 0)
        partners(s, 1, 0)
        free_staging(s, 0, 0)
        t = term(g, (4, 5), cu, ncu).reshape(2, re, ncu)
        tu1[st, 0] = bf(t[:, :hr])
        tu1[st, 1] = bf(t[:, hr:])
        send(s, 0, 0)

    def y1(s):
        g, cu, cy, sl, st = place(s)
        free_staging(s, 1, 0)
        ty1[st] = bf(term(g, (1, 3, 5, 7), cy, ncy)).reshape(4, re, ncy)
        send(s, 1, 0)

    def u2(s):
        g, cu, cy, sl, st = place(s)
        arrived(s, 0, 0)
        partners(s, 0, 1)
        free_staging(s, 0, 1)
        t = term(g, (2, 3), cu, ncu).reshape(2, re, ncu)
        tu2[st, 0, :, :hr] = bf(t[:, :hr] + f32(lu1[sl, 0]))
        tu2[st, 0, :, hr:] = bf(t[:, hr:])
        t = term(g, (6, 7), cu, ncu).reshape(2, re, ncu)
        tu2[st, 1, :, :hr] = bf(t[:, :hr])
        tu2[st, 1, :, hr:] = bf(t[:, hr:] + f32(lu1[sl, 1]))
        send(s, 0, 1)

    def y2(s):
        g, cu, cy, sl, st = place(s)
        arrived(s, 1, 0)
        free_staging(s, 1, 1)
        t = term(g, (4,), cy, ncy) + f32(ly1[sl, 2])
        ty2[st, 0] = bf(t[:hr])
        ty2[st, 1] = bf(t[hr:])
        send(s, 1, 1)

    def u3(s):
        g, cu, cy, sl, st = place(s)
        arrived(s, 0, 1)
        free_staging(s, 0, 2)
        tu3[st] = bf(term(g, (1,), cu, ncu) + f32(lu2[sl, 0, 1]) + f32(lu2[sl, 1, 1]))
        send(s, 0, 2)

    def y3(s):
        g, cu, cy, sl, st = place(s)
        arrived(s, 1, 1)
        free_staging(s, 1, 2)
        t = term(g, (2, 6), cy, ncy)
        a, b = t[:re] + f32(ly1[sl, 1]), t[re:] + f32(ly1[sl, 3])
        ty3[st, 0, :hr] = bf(a[:hr] + f32(ly2[sl, 0]))
        ty3[st, 0, hr:] = bf(a[hr:])
        ty3[st, 1, :hr] = bf(b[:hr])
        ty3[st, 1, hr:] = bf(b[hr:] + f32(ly2[sl, 1]))
        send(s, 1, 2)

    def u4(s):
        g, cu, cy, sl, st = place(s)
        arrived(s, 0, 2)
        partners(s, 0, 2)
        finish(s, 0, term(g, (0,), cu, ncu) + f32(lu2[sl, 0, 0]) + f32(lu2[sl, 1, 0]) + f32(lu3[sl]))

    def y4(s):
        g, cu, cy, sl, st = place(s)
        arrived(s, 1, 2)
        finish(s, 1, term(g, (0,), cy, ncy) + f32(ly1[sl, 0]) + f32(ly3[sl, 0]) + f32(ly3[sl, 1]))

    def fcopy(s, k):
        g, cu, cy, _, st = place(s)
        start, size = ((cu, ncu), (cy, ncy))[k]
        r = pl.ds(pl.multiple_of((g // 2) * re, 8), re)
        cols = pl.ds(pl.multiple_of(role * half + start, LANES), size)
        c = lax.rem(s, CHUNKS)
        return remote(tq.at[c, :, pl.ds(k * ncu, size)], out.at[r, cols], fsend.at[c, k], frecv.at[g // 2], "P")

    def finish(s, k, total):
        g, cu, cy, _, st = place(s)
        c = lax.rem(s, CHUNKS)
        start, size = ((cu, ncu), (cy, ncy))[k]
        piece = tq.at[c, :, pl.ds(k * ncu, size)]

        @pl.when(g == 2)
        def _():
            sent(piece, fsend.at[c, k])

        @pl.when(lax.rem(g, 2) == 0)
        def _():
            piece[...] = bf(total)

        @pl.when((g == 1) | (g == 2))
        def _():
            fcopy(s - CHUNKS * (2 - g), k).start()

        @pl.when(lax.rem(g, 2) == 1)
        def _():
            r = pl.ds(pl.multiple_of((g // 2) * re, 8), re)
            out[r, pl.ds(pl.multiple_of(role * half + start, LANES), size)] = bf(total)

    def reduce_step(i):
        @pl.when(i == 0)
        def _():
            sent(w.at[pl.ds(0, width), pl.ds(0, quarter)], drecv)
            load_w.wait()

        @pl.when(i == steps)
        def _():
            for k, (_, r, (_, c)) in enumerate(kinds):
                blocks = sum(kind(name) == kinds[k] for name in msgs) * r // rows
                sent(xl.at[OWN, pl.ds(0, blocks), :, pl.ds(0, c)], gsend.at[k])
            sent(w.at[pl.ds(0, width), pl.ds(0, quarter)], wsend)
            sent(w.at[pl.ds(0, width), pl.ds(0, quarter)], dsend)
            sent(hid.at[:, :, pl.ds(0, width)], hsend)

        for (a, b), stage in zip(STAGES, (u1, y1, u2, y2, u3, y3, u4, y4), strict=True):
            lag = LAGS[a][b]

            @pl.when((i >= lag) & (i < steps + lag))
            def _():
                stage(i - lag)

    reductions = [k for k, (_, kind) in enumerate(steps_) if kind == "B"]

    def body(j, _):
        communicate(j)
        before, here = jnp.int32(0), jnp.int32(0)
        for k in reductions:
            before += (j > k).astype(jnp.int32)
            here += (j == k).astype(jnp.int32)

        @pl.when(here == 0)
        def _():
            work(j - before)

        @pl.when(here == 1)
        def _():
            reduce_step(before)

        return 0

    lax.fori_loop(0, len(steps_) - 1, body, 0)
    for op in steps_[-1][0]:
        do(op)

    for e in range(EPOCHS):
        sent(out.at[pl.ds(0, re), pl.ds(0, half)], frecv.at[e])
    for s in (steps - 2, steps - 1):
        for i, j in STAGES[:-2]:
            left(s, i, j)
    for c in range(CHUNKS):
        for k in range(2):
            sent(tq.at[c, :, pl.ds(k * ncu, (ncu, ncy)[k])], fsend.at[c, k])


def solution(mesh):
    n = mesh.shape["tp"]

    def step(x, w_gate, w_up, w_down):
        (rows, depth), width = x.shape, w_gate.shape[1]
        order = plan(depth, rows, width)
        msgs = gather_messages(depth, rows)[0]
        re, half = rows // EPOCHS, depth // 2
        hr, unit = re // 2, depth // 28
        ncu, ncy = 8 * unit // CHUNKS, 6 * unit // CHUNKS
        pieces = half // 2 // 256
        tasks = 4 * EPOCHS
        two = 2
        pieces_of_sums = (two, two, hr, ncu), (two, two, re, ncu), (re, ncu), (4, re, ncy), (two, hr, ncy), (two, re, ncy)
        vmem = lambda *shape: pltpu.VMEM(shape, x.dtype)
        dma = lambda *shape: pltpu.SemaphoreType.DMA(shape)
        return pl.pallas_call(
            functools.partial(kernel, n, order, msgs),
            out_shape=(pltpu.VMEM(x.shape, x.dtype), jax.ShapeDtypeStruct((2, n // 2, rows, depth), x.dtype)),
            in_specs=[pl.BlockSpec(memory_space=pl.ANY)] * 4,
            out_specs=(pl.BlockSpec(memory_space=pltpu.VMEM), pl.BlockSpec(memory_space=pl.ANY)),
            scratch_shapes=[
                vmem(3, depth, 2 * LANES),
                vmem(2 * width, half),
                vmem(two, 4 * re, depth),
                vmem(EPOCHS * n, re, 2 * width),
                *(vmem(NB, *p) for p in pieces_of_sums),
                *(vmem(two, *p) for p in pieces_of_sums),
                vmem(CHUNKS, re, ncu + ncy),
                dma(len(send_kinds(msgs))),
                dma(len(arrivals_of(*gather_messages(depth, rows))[1])),
                dma(2),
                dma(3),
                pltpu.SemaphoreType.DMA,
                pltpu.SemaphoreType.DMA,
                dma(pieces),
                pltpu.SemaphoreType.DMA,
                pltpu.SemaphoreType.DMA,
                pltpu.SemaphoreType.DMA,
                dma(tasks, 3),
                dma(two, two, 3),
                dma(FLAGS, two, 3),
                dma(CHUNKS, two),
                dma(EPOCHS),
            ],
            compiler_params=pltpu.CompilerParams(
                collective_id=0, has_side_effects=True, vmem_limit_bytes=VLIM
            ),
        )(x, w_gate, w_up, w_down)[0]

    return jax.shard_map(
        step,
        mesh=mesh,
        in_specs=(P(("dp", "tp"), None), P(None, "tp"), P(None, "tp"), P("tp", None)),
        out_specs=P(("dp", "tp"), None),
        check_vma=False,
    )
```

```python
import functools
import math

import jax
import jax.numpy as jnp
from jax import lax
from jax.experimental import pallas as pl
from jax.experimental.pallas import tpu as pltpu
from jax.sharding import PartitionSpec as P

MESH = pl.DeviceIdType.MESH
LANES = 128
EPOCHS = 2
OWN, OTHER = 0, 1
TASK_SLOTS = (0, 1, 2, 6), (3, 7, 4, 5)
PARTS = ((1,), (2, 6), (0,)), ((3, 7, 4, 5),)
GROUP_TILES = 3
NB = 10
FLAGS = 7
CHUNKS = 4
LAGS = (0, 1, 3, 6), (0, 2, 4, 6)
STAGE_US = (0.6, 1.0, 0.57, 0.61), (0.98, 0.48, 0.61, 0.52)
LINKS = ("NS", "NS", "U"), ("U", "NS", "NS")
SHARE = (1, 2, 1), (4, 0.5, 1)
STAGES = [(i, j) for j in range(4) for i in range(2)]
VLIM = 64600000


FIRST_U, BY_PARTNER = (30, 29), 6
TUNE = {'due_w': (-2685, 675), 'due_f': (-5900, 2080), 'due_p': 1315, 'due_h': (270, 590, 1590, 7110, 5130, 13430, 15010, 26350), 'backlog': 11, 'prefer': 24, 'phase': (0, 0, 2, 1.5), 'hb': 1190, 'blp': 10}


def columns(depth):
    t, (own, other) = depth // 56, FIRST_U
    end = 56 - BY_PARTNER
    return {
        OWN: ((0, own * t), (own * t, (56 - own) * t), None),
        OTHER: ((0, other * t), (other * t, (end - other) * t), (end * t, BY_PARTNER * t)),
    }


def gather_messages(depth, rows):
    msgs, deps = {}, {}
    re = rows // EPOCHS
    cols = columns(depth)

    def add(name, link, cls, src, dst, r, c, dep):
        msgs[name] = (link, cls, src, dst, r, c)
        deps[name] = dep

    for e in range(EPOCHS):
        every, a, b = (e * re, re), (e * re, re // 2), (e * re + re // 2, re // 2)
        add(("P1", OTHER, e), "P", OWN, 0, 0, every, cols[OTHER][0], [])
        add(("P2", OTHER, e), "P", OWN, 0, 0, every, (cols[OTHER][1][0], depth - cols[OTHER][1][0]), [])
        for cls in (OWN, OTHER):
            u, y, _ = cols[cls]
            m = lambda name: (name, cls, e)
            own_u = [] if cls == OWN else [("P1", OTHER, e)]
            own_y = [] if cls == OWN else [("P2", OTHER, e)]
            add(m("U1"), "U", cls, 0, 1, every, u, own_u)
            add(m("N1"), "N", cls, 0, 6, every, u, own_u)
            add(m("S1"), "S", cls, 0, 2, every, u, own_u)
            add(m("U2"), "U", cls, 0, 1, every, y, own_y)
            add(m("N2"), "N", cls, 0, 6, every, y, own_y)
            add(m("S2"), "S", cls, 0, 2, every, y, own_y)
            add(m("N3"), "N", cls, 1, 7, every, u, [m("U1")])
            add(m("S3"), "S", cls, 1, 3, every, u, [m("U1")])
            add(m("N4"), "N", cls, 6, 4, a, u, [m("N1")])
            add(m("S4"), "S", cls, 2, 4, b, u, [m("S1")])
            add(m("N5"), "N", cls, 6, 4, a, y, [m("N2")])
            add(m("S5"), "S", cls, 2, 4, b, y, [m("S2")])
            add(m("U3"), "U", cls, 6, 7, every, y, [m("N2")])
            add(m("U4"), "U", cls, 2, 3, every, y, [m("S2")])
            add(m("N6"), "N", cls, 7, 5, a, u, [m("N3")])
            add(m("S6"), "S", cls, 3, 5, b, u, [m("S3")])
            add(m("U5"), "U", cls, 4, 5, a, y, [m("N5")])
            add(m("U6"), "U", cls, 4, 5, b, y, [m("S5")])
        last = {1: ["U2"], 6: ["N2"], 2: ["S2"], 7: ["U3"], 3: ["U4"], 4: ["N5", "S5"], 5: ["U5", "U6"]}
        for s, need in last.items():
            add((f"F{s}", OTHER, e), "P", OWN, s, s, every, cols[OTHER][2], [(n, OWN, e) for n in need])
    return msgs, deps


def kind_of(message):
    to, cls, _, _, (_, r), cols = message
    return "P" if to == "P" else cls, r, cols


def send_kinds(msgs):
    return sorted({kind_of(m) for m in msgs.values()}, key=str)


def arrivals_of(msgs, deps):
    handed_on = set().union(*deps.values())
    key = {m: m if m in handed_on else (OTHER if v[0] == "P" else v[1], m[2], v[3]) for m, v in msgs.items()}
    order = {k: i for i, k in enumerate(dict.fromkeys(key.values()))}
    return key, order


def plan(depth, rows, width):
    rate, delay, tile_us, gt = 46.6e3, 2.3, 1.48, GROUP_TILES
    due_w, due_f, due_p, due_h, backlog = (TUNE[k] for k in ("due_w", "due_f", "due_p", "due_h", "backlog"))
    msgs, deps = gather_messages(depth, rows)
    pending = {name: set(d) for name, d in deps.items()}
    lack = {}
    for name, (link, cls, src, dst, r, c) in msgs.items():
        where = (OTHER if link == "P" else cls, name[2], dst)
        lack.setdefault(where, set()).add(name)
    pieces = depth // 4 // 256
    tasks = [(cls, e, h) for e in range(EPOCHS) for cls in (OWN, OTHER) for h in range(2)]
    subs = width // LANES // gt
    re, unit = rows // EPOCHS, depth // 28
    ncu, ncy = 8 * unit // CHUNKS, 6 * unit // CHUNKS
    nsteps = 2 * EPOCHS * CHUNKS
    copies = {}
    for i, (name, (link, cls, _, dst, (_, r), (_, c))) in enumerate(msgs.items()):
        e = name[2]
        if name[0][0] == "P":
            rank = due_p * e
        elif name[0][0] == "F":
            rank = due_f[e] + (15 if dst in TASK_SLOTS[1] else 0)
        else:
            rank = TUNE["phase"][2 * e + cls] * 1000 + i
        copies[name] = (link, r * c * 2, rank)
    for k in range(pieces):
        copies["W", k] = ("P", width * 256 * 2, due_w[0] + due_w[1] * k)
    for t in range(len(tasks)):
        for part, slots in enumerate(PARTS[t % 2]):
            due = due_h[t + 1] + 10 * t + 11 + part + TUNE["hb"] if part else due_h[t] + 10 * t
            copies["H", t, part] = ("P", len(slots) * re * width * 2, due)
    free = dict.fromkeys("NSUPC", 0.0)
    avail = [n for n in msgs if not pending[n]] + [("W", k) for k in range(pieces)]
    now, arrivals = 0.0, []
    arrived = {}
    steps, ops = [], []
    loaded = {}
    task = sub = it = forwarded = 0

    def emit(*op):
        ops.append(op)

    def post(link, nbytes, what):
        free[link] = max(now, free[link]) + nbytes / (rate if link != "C" else 300e3)
        arrived[what] = free[link] + delay
        if what[0] not in "DHBE":
            arrivals.append((free[link] + delay, what))

    def issue():
        for n in sorted(avail, key=lambda n: copies[n][2]):
            link, nbytes, _ = copies[n]
            if free[link] - now < (TUNE["blp"] if link == "P" else backlog):
                avail.remove(n)
                emit(*(("wsend", n[1]) if n[0] == "W" else ("hsend", *n[1:]) if n[0] == "H" else ("send", n)))
                post(link, nbytes, n)
        for k in range(task, min(task + 2, len(tasks))):
            cls, e, h = tasks[k]
            for i, s in enumerate(TASK_SLOTS[h]):
                if (k, i) not in loaded and not lack.get((cls, e, s)):
                    loaded[k, i] = now + 1.5
                    emit("load", k, i)

    INF = 1e9

    def active():
        return [(i, j, it - LAGS[i][j]) for i, j in STAGES if 0 <= it - LAGS[i][j] < nsteps]

    def waits(i, j):
        return [("B", i, j - 1, part) for part in range(len(LINKS[i][j - 1]))] if j else []

    def b_ready():
        t, offset = 0.0, 0.0
        if it < nsteps and it % CHUNKS == 0:
            g = it // CHUNKS
            e, cls = g // 2, 1 - g % 2
            if task <= e * 4 + cls * 2 + 1 or forwarded < pieces:
                return INF
            t = max(arrived.get(("H", 2 * g + k, 0), INF) for k in range(2))
            if it == 0:
                t = max(t, max(arrived["D", k] for k in range(pieces)))
        for i, j, s in active():
            t = max([t] + [arrived.get((*q, s), now + 5) - offset for q in waits(i, j)])
            offset += STAGE_US[i][j]
        return t

    while task < len(tasks) or it < nsteps + LAGS[1][3]:
        issue()
        for a in sorted((a for a in arrivals if a[0] <= now), key=lambda a: a[0]):
            arrivals.remove(a)
            what = a[1]
            now += 0.03
            emit("recv", what)
            if what[0] == "W":
                emit("forward", what[1])
                forwarded += 1
                post("C", width * 256 * 2, ("D", what[1]))
            else:
                for s in lack.values():
                    s.discard(what)
                for n in msgs:
                    if what in pending[n]:
                        pending[n].discard(what)
                        if not pending[n]:
                            avail.append(n)
            issue()
        tile_at = INF
        if task < len(tasks) and all((task, i) in loaded for i in range(4)):
            tile_at = max(loaded[task, i] for i in range(4))
        b_at = b_ready() if it < nsteps + LAGS[1][3] else INF
        choice = None
        if b_at <= now and tile_at <= now:
            choice = "B" if min(free["N"], free["U"]) - now < TUNE["prefer"] else "T"
        elif b_at <= now:
            choice = "B"
        elif tile_at <= now:
            choice = "T"
        if choice == "T":
            steps.append((ops, "T"))
            ops = []
            now += gt * tile_us
            sub += 1
            if sub == subs:
                avail.extend(("H", task, part) for part in range(len(PARTS[task % 2])))
                task, sub = task + 1, 0
            continue
        if choice == "B":
            steps.append((ops, "B"))
            ops = []
            for i, j, s in active():
                need = [(*q, s) for q in waits(i, j)]
                if s % CHUNKS == 0 and (i, j) in ((0, 1), (0, 3)):
                    need.append(("H", 2 * (s // CHUNKS), 1 if j == 1 else 2))
                now = max([now] + [arrived[q] for q in need]) + STAGE_US[i][j]
                for part, to in enumerate(LINKS[i][j] if j < 3 else ""):
                    post(to, 2 * SHARE[i][j] * re * (ncu, ncy)[i], ("B", i, j, part, s))
                if j == 3 and s // CHUNKS in (1, 2):
                    post("P", 2 * re * (ncu, ncy)[i], ("E", i, s))
            now += 0.3
            it += 1
            continue
        times = [a[0] for a in arrivals] + [t for t in (tile_at, b_at) if now < t < INF]
        if avail:
            times.append(min(max(now + 0.3, free[copies[n][0]] - (TUNE["blp"] if copies[n][0] == "P" else backlog) + 0.1) for n in avail))
        now = max(now, min(times))
    assert not avail and not arrivals, (avail, arrivals)
    steps.append((ops, ""))
    return steps


def kernel(n, steps_, msgs, x_hbm, gate_hbm, up_hbm, down_hbm, out, xl, gbuf, w, xbuf, hid,
           lu1, lu2, lu3, ly1, ly2, ly3, tu1, tu2, tu3, ty1, ty2, ty3, tq,
           gsend, grecv, xsem, gusem, wosem, wsend, wrecv, dsend, drecv, hsend, hrecv,
           bsend, brecv, fsend, frecv):
    rows, depth = x_hbm.shape
    slots = n // 2
    width = gate_hbm.shape[1]
    re, half = rows // EPOCHS, depth // 2
    quarter, hr = half // 2, re // 2
    tiles = width // LANES
    pieces = quarter // 256
    unit = depth // 28
    ncu, ncy = 8 * unit // CHUNKS, 6 * unit // CHUNKS
    tasks = [(cls, e, h) for e in range(EPOCHS) for cls in (OWN, OTHER) for h in range(2)]
    total_tiles = len(tasks) * tiles
    steps = 2 * EPOCHS * CHUNKS

    side = math.isqrt(n)
    me, dp = lax.axis_index("tp"), lax.axis_index("dp")
    x, y = me // side, me % side
    role, core = ((x + 1) // 2) % 2, dp % 2
    link = {
        "N": {"tp": x * side + (y + 1) % side},
        "S": {"tp": x * side + (y + side - 1) % side},
        "U": {"tp": (side - 1 - x) * side + y},
        "P": {"tp": (x + 1 - 2 * (x % 2)) * side + y},
        "C": {"dp": dp + 1 - 2 * core},
    }

    def remote(src, dst, ssem, rsem, to):
        return pltpu.make_async_remote_copy(
            src_ref=src, dst_ref=dst, send_sem=ssem, recv_sem=rsem, device_id=link[to], device_id_type=MESH
        )

    def sent(ref, sem):
        pltpu.make_async_copy(ref, ref, sem).wait()

    def signal(sem, to):
        pl.semaphore_signal(sem, inc=1, device_id=link[to], device_id_type=MESH)

    barrier = pltpu.get_barrier_semaphore()
    for to in link:
        signal(barrier, to)

    key, arrival = arrivals_of(msgs, gather_messages(depth, rows)[1])
    kinds = send_kinds(msgs)

    def kind(name):
        return kind_of(msgs[name])

    def source(cls, slot):
        return x_hbm if cls == OWN and slot == 0 else xl.at[cls, slot]

    def gcopy(name):
        to, cls, src, dst, (r, nr), (c, nc) = msgs[name]
        there = OTHER if to == "P" else cls
        block = (pl.ds(r, nr), pl.ds(c, nc))
        return remote(
            source(cls, src).at[block], xl.at[(there, dst, *block)], gsend.at[kinds.index(kind(name))], grecv.at[arrival[key[name]]], to
        )

    def xload(t, i):
        cls, e, h = tasks[t]
        src = source(cls, TASK_SLOTS[h][i]).at[pl.ds(e * re, re)]
        return pltpu.make_async_copy(src, xbuf.at[t % 2, pl.ds(i * re, re)], xsem.at[t % 2])

    def load_tile(k):
        slot = lax.rem(k, 3)
        cols = pl.ds(pl.multiple_of(lax.rem(k, tiles) * LANES, LANES), LANES)
        return (
            pltpu.make_async_copy(gate_hbm.at[:, cols], gbuf.at[slot, :, pl.ds(0, LANES)], gusem.at[slot]),
            pltpu.make_async_copy(up_hbm.at[:, cols], gbuf.at[slot, :, pl.ds(LANES, LANES)], gusem.at[slot]),
        )

    def wcopy(k):
        there = pl.ds(pl.multiple_of(core * quarter + k * 256, LANES), 256)
        here = pl.ds(pl.multiple_of((1 - role) * half + core * quarter + k * 256, LANES), 256)
        return remote(down_hbm.at[:, here], w.at[pl.ds(width, width), there], wsend, wrecv.at[k], "P")

    def dcopy(k, whose):
        cols = pl.ds(pl.multiple_of(whose * quarter + k * 256, LANES), 256)
        block = w.at[pl.ds(width, width), cols]
        return remote(block, block, dsend, drecv, "C")

    def hcopy(t, part, slot):
        cls, e, _ = tasks[t]
        src = hid.at[(2 * e + 1 - cls) * slots + slot, :, pl.ds(0, width)]
        dst = hid.at[(2 * e + cls) * slots + slot, :, pl.ds(width, width)]
        return remote(src, dst, hsend, hrecv.at[t // 2, part + 3 * (t % 2)], "P")

    def do(op):
        kind, what = op[0], op[1]
        if kind == "send":
            gcopy(what).start()
        elif kind == "recv" and what[0] == "W":
            wcopy(what[1]).wait_recv()
        elif kind == "recv":
            if key[what] == what:
                gcopy(what).wait_recv()
        elif kind == "load":
            cls, e, h = tasks[what]
            slot = TASK_SLOTS[h][op[2]]
            rest = sum(math.prod(b for _, b in m[4:]) for name, m in msgs.items() if key[name] == (cls, e, slot))
            if rest:
                filled = xl.at[cls, slot, pl.ds(e * re, re), pl.ds(0, rest // re)]
                sent(filled, grecv.at[arrival[cls, e, slot]])
            xload(what, op[2]).start()
        elif kind == "wsend":
            wcopy(what).start()
        elif kind == "forward":
            dcopy(what, core).start()
        elif kind == "hsend":
            for slot in PARTS[what % 2][op[2]]:
                hcopy(what, op[2], slot).start()

    def communicate(j):
        for k, (ops, _) in enumerate(steps_):
            if ops:

                @pl.when(j == k)
                def _():
                    for op in ops:
                        do(op)

    def tile(k):
        t, i, slot = k // tiles, lax.rem(k, tiles), lax.rem(k, 3)
        cls, e, h = lax.rem(t // 2, 2), t // 4, lax.rem(t, 2)
        b = lax.rem(t, 2)

        @pl.when(i == 0)
        def _():
            sent(xbuf.at[b], xsem.at[b])

        sent(gbuf.at[slot], gusem.at[slot])

        @pl.when(k + 2 < total_tiles)
        def _():
            for c in load_tile(k + 2):
                c.start()

        acc = jnp.dot(xbuf[b], gbuf[slot], preferred_element_type=jnp.float32)
        gate, up = acc[:, :LANES], acc[:, LANES:]
        h_tile = (jax.nn.silu(gate) * up).astype(hid.dtype)
        cols = pl.ds(pl.multiple_of(i * LANES, LANES), LANES)
        for j in range(4):
            place = TASK_SLOTS[0][j] + h * (TASK_SLOTS[1][j] - TASK_SLOTS[0][j])
            hid[(2 * e + 1 - cls) * slots + place, :, cols] = h_tile[j * re : (j + 1) * re]

    def work(g):
        def one(i, _):
            tile(g * GROUP_TILES + i)
            return 0

        lax.fori_loop(0, GROUP_TILES, one, 0)

    pl.semaphore_wait(barrier, len(link))
    for c in load_tile(0) + load_tile(1):
        c.start()
    load_w = pltpu.make_async_copy(
        down_hbm.at[:, pl.ds(pl.multiple_of(role * half, LANES), half)], w.at[pl.ds(0, width)], wosem
    )
    load_w.start()

    def term(g, which, start, size):
        if which == tuple(range(which[0], which[0] + len(which))):
            lhs = hid[pl.ds(g * slots + which[0], len(which))].reshape(len(which) * re, 2 * width)
        else:
            lhs = jnp.concatenate([hid[g * slots + s] for s in which], axis=0)
        return jnp.dot(lhs, w[:, pl.ds(pl.multiple_of(start, LANES), size)], preferred_element_type=jnp.float32)

    f32 = lambda v: v.astype(jnp.float32)
    bf = lambda v: v.astype(jnp.bfloat16)

    def place(s):
        c = lax.rem(s, CHUNKS)
        return s // CHUNKS, c * ncu, 8 * unit + c * ncy, lax.rem(s, NB), lax.rem(s, 2)

    staging, landing = ((tu1, tu2, tu3), (ty1, ty2, ty3)), ((lu1, lu2, lu3), (ly1, ly2, ly3))

    def send(s, i, j):
        _, _, _, sl, st = place(s)
        for part, to in enumerate(LINKS[i][j]):
            src, dst = staging[i][j].at[st], landing[i][j].at[sl]
            if len(LINKS[i][j]) > 1:
                src, dst = src.at[part], dst.at[part]
            remote(src, dst, bsend.at[st, i, j], brecv.at[lax.rem(s, FLAGS), i, j], to).start()

    def left(s, i, j):
        st = lax.rem(s, 2)
        sent(staging[i][j].at[st], bsend.at[st, i, j])

    def free_staging(s, i, j):
        @pl.when(s >= 2)
        def _():
            left(s - 2, i, j)

    def arrived(s, i, j):
        _, _, _, sl, _ = place(s)
        sent(landing[i][j].at[sl], brecv.at[lax.rem(s, FLAGS), i, j])

    def partners(s, h, part):
        g = s // CHUNKS

        @pl.when(lax.rem(s, CHUNKS) == 0)
        def _():
            some = pl.ds(g * slots, len(PARTS[h][part]))
            sent(hid.at[some, :, pl.ds(width, width)], hrecv.at[g, part + 3 * h])

    def u1(s):
        g, cu, cy, sl, st = place(s)

        partners(s, 0, 0)
        partners(s, 1, 0)
        free_staging(s, 0, 0)
        t = term(g, (4, 5), cu, ncu).reshape(2, re, ncu)
        tu1[st, 0] = bf(t[:, :hr])
        tu1[st, 1] = bf(t[:, hr:])
        send(s, 0, 0)

    def y1(s):
        g, cu, cy, sl, st = place(s)
        free_staging(s, 1, 0)
        ty1[st] = bf(term(g, (1, 3, 5, 7), cy, ncy)).reshape(4, re, ncy)
        send(s, 1, 0)

    def u2(s):
        g, cu, cy, sl, st = place(s)
        arrived(s, 0, 0)
        partners(s, 0, 1)
        free_staging(s, 0, 1)
        t = term(g, (2, 3), cu, ncu).reshape(2, re, ncu)
        tu2[st, 0, :, :hr] = bf(t[:, :hr] + f32(lu1[sl, 0]))
        tu2[st, 0, :, hr:] = bf(t[:, hr:])
        t = term(g, (6, 7), cu, ncu).reshape(2, re, ncu)
        tu2[st, 1, :, :hr] = bf(t[:, :hr])
        tu2[st, 1, :, hr:] = bf(t[:, hr:] + f32(lu1[sl, 1]))
        send(s, 0, 1)

    def y2(s):
        g, cu, cy, sl, st = place(s)
        arrived(s, 1, 0)
        free_staging(s, 1, 1)
        t = term(g, (4,), cy, ncy) + f32(ly1[sl, 2])
        ty2[st, 0] = bf(t[:hr])
        ty2[st, 1] = bf(t[hr:])
        send(s, 1, 1)

    def u3(s):
        g, cu, cy, sl, st = place(s)
        arrived(s, 0, 1)
        free_staging(s, 0, 2)
        tu3[st] = bf(term(g, (1,), cu, ncu) + f32(lu2[sl, 0, 1]) + f32(lu2[sl, 1, 1]))
        send(s, 0, 2)

    def y3(s):
        g, cu, cy, sl, st = place(s)
        arrived(s, 1, 1)
        free_staging(s, 1, 2)
        t = term(g, (2, 6), cy, ncy)
        a, b = t[:re] + f32(ly1[sl, 1]), t[re:] + f32(ly1[sl, 3])
        ty3[st, 0, :hr] = bf(a[:hr] + f32(ly2[sl, 0]))
        ty3[st, 0, hr:] = bf(a[hr:])
        ty3[st, 1, :hr] = bf(b[:hr])
        ty3[st, 1, hr:] = bf(b[hr:] + f32(ly2[sl, 1]))
        send(s, 1, 2)

    def u4(s):
        g, cu, cy, sl, st = place(s)
        arrived(s, 0, 2)
        partners(s, 0, 2)
        finish(s, 0, term(g, (0,), cu, ncu) + f32(lu2[sl, 0, 0]) + f32(lu2[sl, 1, 0]) + f32(lu3[sl]))

    def y4(s):
        g, cu, cy, sl, st = place(s)
        arrived(s, 1, 2)
        finish(s, 1, term(g, (0,), cy, ncy) + f32(ly1[sl, 0]) + f32(ly3[sl, 0]) + f32(ly3[sl, 1]))

    def fcopy(s, k):
        g, cu, cy, _, st = place(s)
        start, size = ((cu, ncu), (cy, ncy))[k]
        r = pl.ds(pl.multiple_of((g // 2) * re, 8), re)
        cols = pl.ds(pl.multiple_of(role * half + start, LANES), size)
        c = lax.rem(s, CHUNKS)
        return remote(tq.at[c, :, pl.ds(k * ncu, size)], out.at[r, cols], fsend.at[c, k], frecv.at[g // 2], "P")

    def finish(s, k, total):
        g, cu, cy, _, st = place(s)
        c = lax.rem(s, CHUNKS)
        start, size = ((cu, ncu), (cy, ncy))[k]
        piece = tq.at[c, :, pl.ds(k * ncu, size)]

        @pl.when(g == 2)
        def _():
            sent(piece, fsend.at[c, k])

        @pl.when(lax.rem(g, 2) == 0)
        def _():
            piece[...] = bf(total)

        @pl.when((g == 1) | (g == 2))
        def _():
            fcopy(s - CHUNKS * (2 - g), k).start()

        @pl.when(lax.rem(g, 2) == 1)
        def _():
            r = pl.ds(pl.multiple_of((g // 2) * re, 8), re)
            out[r, pl.ds(pl.multiple_of(role * half + start, LANES), size)] = bf(total)

    def reduce_step(i):
        @pl.when(i == 0)
        def _():
            sent(w.at[pl.ds(0, width), pl.ds(0, quarter)], drecv)
            load_w.wait()

        @pl.when(i == steps)
        def _():
            for k, (_, r, (_, c)) in enumerate(kinds):
                blocks = sum(kind(name) == kinds[k] for name in msgs) * r // rows
                sent(xl.at[OWN, pl.ds(0, blocks), :, pl.ds(0, c)], gsend.at[k])
            sent(w.at[pl.ds(0, width), pl.ds(0, quarter)], wsend)
            sent(w.at[pl.ds(0, width), pl.ds(0, quarter)], dsend)
            sent(hid.at[:, :, pl.ds(0, width)], hsend)

        for (a, b), stage in zip(STAGES, (u1, y1, u2, y2, u3, y3, u4, y4), strict=True):
            lag = LAGS[a][b]

            @pl.when((i >= lag) & (i < steps + lag))
            def _():
                stage(i - lag)

    reductions = [k for k, (_, kind) in enumerate(steps_) if kind == "B"]

    def body(j, _):
        communicate(j)
        before, here = jnp.int32(0), jnp.int32(0)
        for k in reductions:
            before += (j > k).astype(jnp.int32)
            here += (j == k).astype(jnp.int32)

        @pl.when(here == 0)
        def _():
            work(j - before)

        @pl.when(here == 1)
        def _():
            reduce_step(before)

        return 0

    lax.fori_loop(0, len(steps_) - 1, body, 0)
    for op in steps_[-1][0]:
        do(op)

    for e in range(EPOCHS):
        sent(out.at[pl.ds(0, re), pl.ds(0, half)], frecv.at[e])
    for s in (steps - 2, steps - 1):
        for i, j in STAGES[:-2]:
            left(s, i, j)
    for c in range(CHUNKS):
        for k in range(2):
            sent(tq.at[c, :, pl.ds(k * ncu, (ncu, ncy)[k])], fsend.at[c, k])


def solution(mesh):
    n = mesh.shape["tp"]

    def step(x, w_gate, w_up, w_down):
        (rows, depth), width = x.shape, w_gate.shape[1]
        order = plan(depth, rows, width)
        msgs = gather_messages(depth, rows)[0]
        re, half = rows // EPOCHS, depth // 2
        hr, unit = re // 2, depth // 28
        ncu, ncy = 8 * unit // CHUNKS, 6 * unit // CHUNKS
        pieces = half // 2 // 256
        tasks = 4 * EPOCHS
        two = 2
        pieces_of_sums = (two, two, hr, ncu), (two, two, re, ncu), (re, ncu), (4, re, ncy), (two, hr, ncy), (two, re, ncy)
        vmem = lambda *shape: pltpu.VMEM(shape, x.dtype)
        dma = lambda *shape: pltpu.SemaphoreType.DMA(shape)
        return pl.pallas_call(
            functools.partial(kernel, n, order, msgs),
            out_shape=(pltpu.VMEM(x.shape, x.dtype), jax.ShapeDtypeStruct((2, n // 2, rows, depth), x.dtype)),
            in_specs=[pl.BlockSpec(memory_space=pl.ANY)] * 4,
            out_specs=(pl.BlockSpec(memory_space=pltpu.VMEM), pl.BlockSpec(memory_space=pl.ANY)),
            scratch_shapes=[
                vmem(3, depth, 2 * LANES),
                vmem(2 * width, half),
                vmem(two, 4 * re, depth),
                vmem(EPOCHS * n, re, 2 * width),
                *(vmem(NB, *p) for p in pieces_of_sums),
                *(vmem(two, *p) for p in pieces_of_sums),
                vmem(CHUNKS, re, ncu + ncy),
                dma(len(send_kinds(msgs))),
                dma(len(arrivals_of(*gather_messages(depth, rows))[1])),
                dma(2),
                dma(3),
                pltpu.SemaphoreType.DMA,
                pltpu.SemaphoreType.DMA,
                dma(pieces),
                pltpu.SemaphoreType.DMA,
                pltpu.SemaphoreType.DMA,
                pltpu.SemaphoreType.DMA,
                dma(tasks // two, 4),
                dma(two, two, 3),
                dma(FLAGS, two, 3),
                dma(CHUNKS, two),
                dma(EPOCHS),
            ],
            compiler_params=pltpu.CompilerParams(
                collective_id=0, has_side_effects=True, vmem_limit_bytes=VLIM
            ),
        )(x, w_gate, w_up, w_down)[0]

    return jax.shard_map(
        step,
        mesh=mesh,
        in_specs=(P(("dp", "tp"), None), P(None, "tp"), P(None, "tp"), P("tp", None)),
        out_specs=P(("dp", "tp"), None),
        check_vma=False,
    )
```
